128 devices in a mesh: gx: 8 (over z_lo, y), gy: 16 (over x, z_hi, core).
Axes of the slice: x: 4, y: 4, z: 4 (z_hi: 2, z_lo: 2; z = z_hi * 2 + z_lo), core: 2. Of those that a mesh axis runs over, the one named last changes fastest.
Arguments:
- cotangent: float32 [256, 1024, 128], P('gx', 'gy'), may hold values from -6 to 6
- speed: float32 [3, 256, 1024, 128], P(None, 'gx', 'gy'), may hold values from 0.05 to 0.45
- coeff: float32 [3, 256, 1024, 128], P(None, 'gx', 'gy'), may hold values from 0.3 to 3
- dirs: int32 [3, 256, 1024], P(None, 'gx', 'gy'), may hold values from 0 to 1
Outputs:
- grad: float32 [256, 1024, 128], P('gx', 'gy')
The draws below stay inside these ranges and needn't reach their ends.
Inputs may be any that keep to these rules, and one draw needn't show every extreme that they name: `dirs`: 0 means the lower cell of a face is upwind, 1 the upper cell.
All inputs are finite; a program needn't handle non-finite values.
Results may differ from the reference program's by a relative error of at most 0.0003.
Values sent between devices are 32-bit elements; how exact they have to be, the bound alone decides.
A program may use at most 128 MiB of HBM per device.

```python
import math
import jax
import jax.numpy as jnp
from jax import lax

NZ = 128
ITERS = 2
NX = 256
NY = 1024


def plant(array, rng, smallest, top_value):
    index_at = [jax.random.randint(jax.random.fold_in(rng, axis), (), 0, length) for axis, length in enumerate(array.shape)]
    main_axis = array.shape.index(max(array.shape))
    next_to = index_at[:main_axis] + [(index_at[main_axis] + 1) % array.shape[main_axis]] + index_at[main_axis + 1:]
    return array.at[tuple(index_at)].set(smallest).at[tuple(next_to)].set(top_value)


def shard_levels(own_key, shape, pieces, smallest, top_value):
    gain = 1.0
    for dim, parts in pieces:
        steps = jax.random.uniform(jax.random.fold_in(jax.random.fold_in(own_key, 6), dim), (parts,), jnp.float32, smallest / len(pieces), top_value / len(pieces))
        gain = gain * jnp.repeat(jnp.exp(steps), shape[dim] // parts).reshape((-1,) + (1,) * (len(shape) - 1 - dim))
    return gain


def scatter_about(rng, dims, width, limit, shards=(), held_as=jnp.bfloat16):
    drawn = width * jax.random.normal(rng, dims, jnp.float32)
    if shards:
        drawn = drawn * shard_levels(rng, dims, shards, -0.22, 0.18)
    return jnp.clip(drawn, -limit, limit).astype(held_as)


def setup_inputs(seed: int = 0) -> dict:
    seeds = jax.random.split(jax.random.key(seed), 5)
    return {
        "cotangent": scatter_about(seeds[0], (NX, NY, NZ), 1.0, 6.0, ((0, 8), (1, 16)), jnp.float32),
        "speed": jnp.clip(jnp.exp(math.log(0.45) - 2.1972245 * jax.random.uniform(seeds[1], (3, NX, NY, NZ), jnp.float32) ** shard_levels(seeds[1], (3, NX, NY, NZ), ((1, 8), (2, 16)), -0.2, 0.2)), 0.05, 0.45),
        "coeff": jnp.clip(jnp.exp(math.log(3.0) - 2.3025851 * jax.random.uniform(seeds[2], (3, NX, NY, NZ), jnp.float32) ** shard_levels(seeds[2], (3, NX, NY, NZ), ((1, 8), (2, 16)), -0.2, 0.2)), 0.3, 3.0),
        "dirs": plant(jax.random.randint(seeds[3], (3, NX, NY), 0, 2), jax.random.fold_in(seeds[3], 1), 0, 1).astype(jnp.int32),
    }


explicit_table = ((0.0, 0.0, 0.0, 0.0), (0.5, 0.0, 0.0, 0.0), (0.25, 0.5, 0.0, 0.0), (0.2, 0.3, 0.5, 0.0))
implicit_table = ((0.0, 0.0, 0.0, 0.0), (0.25, 0.25, 0.0, 0.0), (0.25, 0.25, 0.25, 0.0), (0.15, 0.35, 0.25, 0.25))
section_weights = (0.15, 0.35, 0.25, 0.25)
implicit_diagonal = 0.25
step_length = 1.0


def local_ahead(values, dimension):
    tail = lax.slice_in_dim(values, 1, values.shape[dimension], axis=dimension)
    return jnp.concatenate([tail, jnp.zeros_like(lax.slice_in_dim(values, 0, 1, axis=dimension))], dimension)


def local_behind(values, dimension):
    head = lax.slice_in_dim(values, 0, values.shape[dimension] - 1, axis=dimension)
    return jnp.concatenate([jnp.zeros_like(lax.slice_in_dim(values, 0, 1, axis=dimension)), head], dimension)


def transposed(advected, diffused, velocity, coeff):
    total = jnp.zeros_like(diffused)
    for dimension in range(3):
        flux = coeff[dimension] * (local_ahead(diffused, dimension) - diffused)
        total = total + flux - local_behind(flux, dimension)
        if advected is not None:
            moved = velocity[dimension] * (local_ahead(advected, dimension) - advected)
            upwind_here = velocity[dimension] > 0
            total = total + jnp.where(upwind_here, moved, 0.0)
            total = total + local_behind(jnp.where(upwind_here, 0.0, moved), dimension)
    return total


def solve_section(rhs, velocity, coeff):
    solution = jnp.zeros_like(rhs)
    residual = rhs
    direction = rhs
    norm_now = jnp.sum(residual * residual)
    for iteration in range(ITERS):
        image = direction - implicit_diagonal * step_length * transposed(None, direction, velocity, coeff)
        alpha = norm_now / jnp.sum(direction * image)
        solution = solution + alpha * direction
        residual = residual - alpha * image
        norm_next = jnp.sum(residual * residual)
        direction = residual + (norm_next / norm_now) * direction
        norm_now = norm_next
    return solution


def reference(cotangent, speed, coeff, dirs):
    signs = (1 - 2 * dirs).astype(jnp.float32)
    velocity = speed * signs[..., None]
    section_adjoints = [None, None, None, None]
    for section_index in (3, 2, 1, 0):
        advected = step_length * section_weights[section_index] * cotangent
        diffused = step_length * section_weights[section_index] * cotangent
        for later in range(section_index + 1, 4):
            advected = advected + step_length * explicit_table[later][section_index] * section_adjoints[later]
            diffused = diffused + step_length * implicit_table[later][section_index] * section_adjoints[later]
        source = transposed(advected, diffused, velocity, coeff)
        if section_index > 0:
            section_adjoints[section_index] = solve_section(source, velocity, coeff)
        else:
            section_adjoints[section_index] = source
    return cotangent + section_adjoints[0] + section_adjoints[1] + section_adjoints[2] + section_adjoints[3]
```

```python
import functools

import jax
import jax.numpy as jnp
from jax import lax
from jax.experimental import pallas as pl
from jax.experimental.pallas import tpu as pltpu
from jax.sharding import PartitionSpec as P

MESH = pl.DeviceIdType.MESH
F32 = jnp.float32

BX, BY, BZ = 32, 64, 128
OX, OY = 2, 16
EX, EY = BX + 2 * OX, BY + 2 * OY
TOP, BOT = OY, OY + BY
EXT = (EX, EY, BZ)
PARTS = {"zl": 2, "y": 4, "x": 4, "zh": 2, "c": 2}


def offsets(axes):
    found = [{}]
    for axis in axes:
        found = [dict(o, **{axis: i}) for o in found for i in range(PARTS[axis])]
    found = [o for o in found if any(o.values())]

    def distance(o):
        total = 0
        for axis, i in o.items():
            if axis in ("x", "y"):
                total += min(i, 4 - i)
            elif axis == "zh":
                total += 2 * i
            else:
                total += i
        return total

    return sorted(found, key=lambda o: -distance(o))


GROUP_A = offsets(("zl", "zh", "c"))
GROUP_B = offsets(("x", "y"))
EVERYONE = offsets(("x", "y", "zh", "zl", "c"))


def kernel(cot, speed, coeff, dirs, out, cfield, cf, vel, y4, w4, g4, qr4, y3, w3, g3, qr3, y2, w2, t1, t2, b1,
           signs, sums, load_sem, send, recv, ar_send, ar_recv, in_sem, out_sem):
    gx, gy = lax.axis_index("gx"), lax.axis_index("gy")
    place = {"zl": gx // 4, "y": gx % 4, "x": gy // 4, "zh": (gy // 2) % 2, "c": gy % 2}

    def device(offset):
        at = {k: (place[k] + offset[k]) % PARTS[k] if offset.get(k, 0) else place[k] for k in place}
        return {"gx": at["zl"] * 4 + at["y"], "gy": at["x"] * 4 + at["zh"] * 2 + at["c"]}

    def neighbour(sx, sy):
        return {"gx": (gx + sx + 8) % 8, "gy": (gy + sy + 16) % 16}

    lane = lax.broadcasted_iota(jnp.int32, (8, BZ), 1)

    def zero_rim(ref, *lead):
        for x in (0, 1, EX - 2, EX - 1):
            ref[(*lead, x)] = jnp.zeros((EY, BZ), F32)

        def body(x, _):
            ref[(*lead, x, pl.ds(TOP - 8, 8))] = jnp.zeros((8, BZ), F32)
            ref[(*lead, x, pl.ds(BOT, 8))] = jnp.zeros((8, BZ), F32)
            return 0

        lax.fori_loop(OX, OX + BX, body, 0, unroll=8)

    inner = (pl.ds(OX, BX), pl.ds(OY, BY))
    loads = [pltpu.make_async_copy(cot, cfield.at[inner], load_sem.at[0])]
    for d in range(3):
        loads.append(pltpu.make_async_copy(speed.at[d], vel.at[(d, *inner)], load_sem.at[1 + d]))
    for d in range(3):
        loads.append(pltpu.make_async_copy(coeff.at[d], cf.at[(d, *inner)], load_sem.at[4 + d]))
    for load in loads:
        load.start()

    zero_rim(cfield)
    for d in range(3):
        zero_rim(cf, d)
    zero_rim(vel, 0)
    zero_rim(vel, 1)
    zero_rim(y4)

    barrier = pltpu.get_barrier_semaphore()
    friends = [neighbour(sx, sy) for sx in (-1, 0, 1) for sy in (-1, 0, 1) if sx or sy]
    friends += [device(o) for o in GROUP_A] + [device(o) for o in GROUP_B]
    for friend in friends:
        pl.semaphore_signal(barrier, inc=1, device_id=friend, device_id_type=MESH)

    for k in range(2):
        zero_rim(qr4, k)
    for k in range(3):
        zero_rim(qr3, k)

    signs[...] = jnp.zeros((128, 128), F32)
    for d in range(3):
        signs[pl.ds(32 * d, 32), pl.ds(0, 64)] = (1 - 2 * dirs[d]).astype(F32)
    signs[...] = signs[...].T
    for load in loads[1:4]:
        load.wait()
    columns = signs[pl.ds(0, 64), :]
    for d in range(3):
        for x in range(BX):
            k = 32 * d + x
            rows = pl.ds(OY, BY)
            vel[d, OX + x, rows] = vel[d, OX + x, rows] * columns[:, k:k + 1]
    loads[0].wait()
    for load in loads[4:]:
        load.wait()

    count = [0]
    edges = {-1: (gx > 0, gy > 0), 1: (gx < 7, gy < 15)}

    def transfer(ref, lead, source, target, sx, sy):
        k = count[0]
        count[0] += 1
        copy = pltpu.make_async_remote_copy(
            src_ref=ref.at[(*lead, *source)], dst_ref=ref.at[(*lead, *target)],
            send_sem=send.at[k], recv_sem=recv.at[k], device_id=neighbour(sx, sy), device_id_type=MESH)
        sends, receives = None, None
        if sx:
            sends, receives = edges[sx][0], edges[-sx][0]
        if sy:
            ys, yr = edges[sy][1], edges[-sy][1]
            sends = ys if sends is None else jnp.logical_and(sends, ys)
            receives = yr if receives is None else jnp.logical_and(receives, yr)
        pl.when(sends)(copy.start)
        return copy, sends, receives

    def finish(copies):
        for copy, sends, receives in copies:
            pl.when(receives)(copy.wait_recv)
            pl.when(sends)(copy.wait_send)

    XS, YS = pl.ds(OX, BX), pl.ds(OY, BY)

    def to_above(ref, lead, axis, width):
        if axis == 0:
            return transfer(ref, lead, (pl.ds(OX + BX - width, width), YS), (pl.ds(OX - width, width), YS), 1, 0)
        return transfer(ref, lead, (XS, pl.ds(BOT - width, width)), (XS, pl.ds(TOP - width, width)), 0, 1)

    def to_below(ref, lead, axis, width):
        if axis == 0:
            return transfer(ref, lead, (pl.ds(OX, width), YS), (pl.ds(OX + BX, width), YS), -1, 0)
        return transfer(ref, lead, (XS, pl.ds(TOP, width)), (XS, pl.ds(BOT, width)), 0, -1)

    def corner(ref, lead, sx, sy):
        xs, xt = (OX + BX - 1, OX - 1) if sx > 0 else (OX, OX + BX)
        ys, yt = (BOT - 1, TOP - 1) if sy > 0 else (TOP, BOT)
        return transfer(ref, lead, (pl.ds(xs, 1), pl.ds(ys, 1)), (pl.ds(xt, 1), pl.ds(yt, 1)), sx, sy)

    def swap(ref, lead):
        return [to_above(ref, lead, 0, 2), to_below(ref, lead, 0, 2), to_above(ref, lead, 1, 2),
                to_below(ref, lead, 1, 2)] + [corner(ref, lead, sx, sy) for sx in (1, -1) for sy in (1, -1)]

    def ahead_z(v):
        rows = v.shape[0]
        at = lax.broadcasted_iota(jnp.int32, (rows, BZ), 1)
        return jnp.where(at == BZ - 1, 0.0, pltpu.roll(v, BZ - 1, 1))

    def behind_z(v):
        rows = v.shape[0]
        at = lax.broadcasted_iota(jnp.int32, (rows, BZ), 1)
        return jnp.where(at == 0, 0.0, pltpu.roll(v, 1, 1))

    def stencil(src, x0, n, segments, emit, advect=True, diffuse=True, unroll=1):
        def start(r, size):
            rows = pl.ds(r, size)
            v = src[x0, rows]
            dx = v - src[x0 - 1, rows]
            parts = [v]
            if diffuse:
                parts.append(cf[0, x0 - 1, rows] * dx)
            if advect:
                parts.append(jnp.minimum(vel[0, x0 - 1, rows], 0.0) * dx)
            return tuple(parts)

        def plane(x, carry):
            done = []
            for (r, size), held in zip(segments, carry):
                rows, up, down = pl.ds(r, size), pl.ds(r + 1, size), pl.ds(r - 1, size)
                v = held[0]
                ahead = src[x + 1, rows]
                dx = ahead - v
                dyu = src[x, up] - v
                dyd = v - src[x, down]
                dz = ahead_z(v) - v
                parts = [ahead]
                dv = fv = None
                if diffuse:
                    fx = cf[0, x, rows] * dx
                    fz = cf[2, x, rows] * dz
                    dv = (fx - held[1]) + (cf[1, x, rows] * dyu - cf[1, x, down] * dyd) + (fz - behind_z(fz))
                    parts.append(fx)
                if advect:
                    u0, u1, u2 = vel[0, x, rows], vel[1, x, rows], vel[2, x, rows]
                    fv = (jnp.maximum(u0, 0.0) * dx + held[-1])
                    fv = fv + (jnp.maximum(u1, 0.0) * dyu + jnp.minimum(vel[1, x, down], 0.0) * dyd)
                    fv = fv + (jnp.maximum(u2, 0.0) * dz + behind_z(jnp.minimum(u2, 0.0) * dz))
                    parts.append(jnp.minimum(u0, 0.0) * dx)
                emit(x, rows, v, fv, dv)
                done.append(tuple(parts))
            return tuple(done)

        carry = tuple(start(r, size) for r, size in segments)
        if unroll >= n:
            for i in range(n):
                carry = plane(x0 + i, carry)
        else:
            lax.fori_loop(x0, x0 + n, plane, carry, unroll=unroll)

    WHOLE = ((OY, BY),)
    INNER = ((OY + 8, BY - 16),)
    STRIPS = ((OY, 8), (BOT - 8, 8))

    def rim_then_inner(run, width):
        run(OX, width, WHOLE, width)
        run(OX + BX - width, width, WHOLE, width)
        run(OX + width, BX - 2 * width, STRIPS, BX)

    def inner_part(run, width):
        n = BX - 2 * width
        run(OX + width, n, INNER, n // 4 if n % 4 == 0 else n // 5)

    def emit_y4(x, rows, v, fv, dv):
        y4[x, rows] = 0.25 * (fv + dv)

    def run_y4(x0, n, segments, unroll):
        stencil(cfield, x0, n, segments, emit_y4, unroll=unroll)

    pl.semaphore_wait(barrier, len(friends))
    first = [to_above(cfield, (), 0, 1), to_below(cfield, (), 0, 1), to_above(cfield, (), 1, 1),
             to_below(cfield, (), 1, 1), to_above(cf, (0,), 0, 2), to_above(cf, (1,), 1, 2),
             to_above(vel, (0,), 0, 1), to_above(vel, (1,), 1, 1)]
    later = [to_above(cf, (pl.ds(1, 2),), 0, 1), to_below(cf, (pl.ds(0, 3),), 0, 1),
             to_above(cf, (0,), 1, 1), to_above(cf, (2,), 1, 1), to_below(cf, (pl.ds(0, 3),), 1, 1),
             corner(cf, (pl.ds(0, 2),), 1, 1), corner(cf, (1,), -1, 1), corner(cf, (0,), 1, -1)]
    for o in GROUP_B:
        pl.semaphore_signal(in_sem, inc=1, device_id=device(o), device_id_type=MESH)
    inner_part(run_y4, 1)
    finish(first)
    rim_then_inner(run_y4, 1)
    moved = swap(y4, ())

    def laplacian(src, dst, x0, n, segments, unroll):
        def emit(x, rows, v, fv, dv):
            dst[x, rows] = -dv

        stencil(src, x0, n, segments, emit, advect=False, unroll=unroll)

    WIDE = ((OY - 8, BY + 16),)

    def clear_outside(ref):
        @pl.when(gx == 0)
        def _():
            ref[OX - 1] = jnp.zeros((EY, BZ), F32)

        @pl.when(gx == 7)
        def _():
            ref[OX + BX] = jnp.zeros((EY, BZ), F32)

        def rows_at(r):
            def body(x, _):
                ref[x, pl.ds(r, 8)] = jnp.zeros((8, BZ), F32)
                return 0
            lax.fori_loop(OX, OX + BX, body, 0, unroll=8)

        pl.when(gy == 0)(lambda: rows_at(TOP - 8))
        pl.when(gy == 15)(lambda: rows_at(BOT))

    def fold(values):
        return jnp.sum(values.reshape(values.shape[0] // 8, 8, BZ), axis=0)

    def moments(y, w):
        def plane(x, carry):
            a0, a1, a2, a3, here = carry
            rows = pl.ds(OY, BY)
            v = y[x, rows]
            ahead = w[x + 1, rows]
            dx = ahead - here
            dy = w[x, pl.ds(OY + 1, BY)] - here
            dz = ahead_z(here) - here
            energy = (cf[0, x, rows] * dx) * dx + (cf[1, x, rows] * dy) * dy + (cf[2, x, rows] * dz) * dz
            return (a0 + fold(v * v), a1 + fold(v * here), a2 + fold(here * here), a3 + fold(energy), ahead)

        zero = jnp.zeros((8, BZ), F32)
        got = lax.fori_loop(OX, OX + BX, plane, (zero, zero, zero, zero, w[OX, pl.ds(OY, BY)]), unroll=4)
        return got[:4]

    def send_sums(r, parts):
        row = jnp.zeros((1, BZ), F32)
        for k, part in enumerate(parts):
            total = jnp.sum(jnp.sum(part, axis=0, keepdims=True), axis=1, keepdims=True)
            row = jnp.where(lane[0:1] == k, total, row)
        sums[r, pl.ds(127, 1)] = row
        for k, o in enumerate(EVERYONE):
            pltpu.make_async_remote_copy(
                src_ref=sums.at[r, pl.ds(127, 1)], dst_ref=sums.at[r, pl.ds(k, 1)],
                send_sem=ar_send.at[r], recv_sem=ar_recv.at[r], device_id=device(o), device_id_type=MESH).start()

    def solve(r):
        pltpu.make_async_remote_copy(
            src_ref=sums.at[r, pl.ds(0, 127)], dst_ref=sums.at[r, pl.ds(0, 127)],
            send_sem=ar_send.at[r], recv_sem=ar_recv.at[r], device_id=device(EVERYONE[0]), device_id_type=MESH).wait()
        row = jnp.sum(sums[r], axis=0, keepdims=True)
        m0, k1, k2, k3 = (
            jnp.broadcast_to(jnp.sum(jnp.where(lane[0:1] == k, row, 0.0), axis=1, keepdims=True), (8, BZ))
            for k in range(4))
        h = 0.25
        alpha = m0 / (m0 + h * k1)
        rho = k1 / m0
        ss = k2 - rho * k1
        sls = k3 - 2.0 * rho * k2 + rho * (rho * k1)
        beta = (alpha * h) * (alpha * h) * (ss / m0)
        under = ss * (1.0 - beta / alpha) + h * sls
        second = jnp.where(under > 0.0, jnp.clip(ss / under, 0.0, 1.0), 0.0)
        return alpha + second * (alpha * h * rho + beta), -second * alpha * h

    def full(scalar, size):
        return jnp.concatenate([scalar] * (size // 8), axis=0)

    def advance(y, w, qr, g, r):
        def emit_q(x, rows, v, fv, dv):
            qr[0, x, rows] = 0.5 * fv - 0.25 * w[x, rows]

        def emit_r(x, rows, v, fv, dv):
            qr[1, x, rows] = 0.5 * fv + 0.25 * dv
            g[x, rows] = dv

        def run_q(x0, n, segments, unroll):
            stencil(y, x0, n, segments, emit_q, diffuse=False, unroll=unroll)

        def run_r(x0, n, segments, unroll):
            stencil(w, x0, n, segments, emit_r, unroll=unroll)

        rim_then_inner(run_q, 2)
        rim_then_inner(run_r, 2)
        copies = swap(qr, (pl.ds(0, 2),))
        inner_part(run_q, 2)
        inner_part(run_r, 2)
        return copies

    def everywhere(fn):
        def body(x, _):
            fn(x, pl.ds(OY - 8, BY + 16))
            return 0
        lax.fori_loop(0, EX, body, 0, unroll=4)

    def block(fn, unroll=4):
        def body(x, _):
            fn(x, pl.ds(OY, BY))
            return 0
        lax.fori_loop(OX, OX + BX, body, 0, unroll=unroll)

    inner_part(functools.partial(laplacian, y4, w4), 1)
    finish(moved)
    finish(later)
    laplacian(y4, w4, OX - 1, 2, WIDE, 2)
    laplacian(y4, w4, OX + BX - 1, 2, WIDE, 2)
    laplacian(y4, w4, OX + 1, BX - 2, ((OY - 8, 16), (BOT - 8, 16)), BX)
    clear_outside(w4)
    parts = moments(y4, w4)
    pl.semaphore_wait(in_sem, len(GROUP_B))
    send_sums(0, parts)
    moved = advance(y4, w4, qr4, g4, 0)
    finish(moved)
    a4, c4 = solve(0)

    def base2(x, rows):
        size = rows.size
        a, c = full(a4, size), full(c4, size)
        qr3[2, x, rows] = (1.4 * y4[x, rows] + a * (0.6 * qr4[0, x, rows] - 0.2 * w4[x, rows])
                           + c * (0.6 * qr4[1, x, rows] + 0.2 * g4[x, rows]))

    block(base2)
    moved2 = swap(qr3, (2,))

    def make_y3(x, rows):
        a, c = full(a4, rows.size), full(c4, rows.size)
        y3[x, rows] = y4[x, rows] + a * qr4[0, x, rows] + c * qr4[1, x, rows]

    everywhere(make_y3)
    laplacian(y3, w3, OX - 1, BX + 2, WIDE, 4)
    clear_outside(w3)
    send_sums(1, moments(y3, w3))
    moved = advance(y3, w3, qr3, g3, 1)
    finish(moved2)
    finish(moved)
    a3, c3 = solve(1)

    def make_y2(x, rows):
        a, c = full(a3, rows.size), full(c3, rows.size)
        y2[x, rows] = qr3[2, x, rows] + a * qr3[0, x, rows] + c * qr3[1, x, rows]

    everywhere(make_y2)
    laplacian(y2, w2, OX - 1, BX + 2, WIDE, 4)
    clear_outside(w2)
    send_sums(2, moments(y2, w2))

    def emit_t1(x, rows, v, fv, dv):
        t1[x - OX, pl.ds(rows.start - OY, rows.size)] = v + 0.5 * fv - 0.25 * w2[x, rows]

    def emit_t2(x, rows, v, fv, dv):
        t2[x - OX, pl.ds(rows.start - OY, rows.size)] = v + 0.5 * fv + 0.25 * dv

    stencil(y2, OX, BX, WHOLE, emit_t1, diffuse=False, unroll=4)
    stencil(w2, OX, BX, WHOLE, emit_t2, unroll=4)

    def base1(x, rows):
        size = rows.size
        a, c, a_, c_ = full(a4, size), full(c4, size), full(a3, size), full(c3, size)
        total = cfield[x, rows] + 0.6 * y4[x, rows]
        total = total + a * (y4[x, rows] + 0.4 * qr4[0, x, rows] - 0.05 * w4[x, rows])
        total = total + c * (w4[x, rows] + 0.4 * qr4[1, x, rows] + 0.05 * g4[x, rows])
        total = total + a_ * (y3[x, rows] + 0.5 * qr3[0, x, rows] - 0.125 * w3[x, rows])
        total = total + c_ * (w3[x, rows] + 0.5 * qr3[1, x, rows] + 0.125 * g3[x, rows])
        b1[x - OX] = total

    block(base1)
    a2, c2 = solve(2)
    stores = []
    for k in range(4):
        planes = pl.ds(8 * k, 8)

        def body(x, _):
            b1[x] = b1[x] + full(a2, BY) * t1[x] + full(c2, BY) * t2[x]
            return 0

        lax.fori_loop(8 * k, 8 * k + 8, body, 0, unroll=4)
        store = pltpu.make_async_copy(b1.at[planes], out.at[planes], out_sem.at[k])
        store.start()
        stores.append(store)
    for store in stores:
        store.wait()


COPIES = 80


def local(cotangent, speed, coeff, dirs):
    ext = pltpu.VMEM(EXT, F32)
    plain = pltpu.VMEM((BX, BY, BZ), F32)

    def stack(n):
        return pltpu.VMEM((n, *EXT), F32)

    anywhere = pl.BlockSpec(memory_space=pl.ANY)
    return pl.pallas_call(
        kernel,
        name="adjoint_step",
        out_shape=jax.ShapeDtypeStruct((BX, BY, BZ), F32),
        in_specs=[anywhere, anywhere, anywhere, pl.BlockSpec(memory_space=pltpu.VMEM)],
        out_specs=anywhere,
        scratch_shapes=[
            ext, stack(3), stack(3), ext, ext, ext, stack(2), ext, ext, ext, stack(3), ext, ext,
            plain, plain, plain, pltpu.VMEM((128, 128), F32), pltpu.VMEM((3, 128, BZ), F32),
            pltpu.SemaphoreType.DMA((7,)), pltpu.SemaphoreType.DMA((COPIES,)), pltpu.SemaphoreType.DMA((COPIES,)),
            pltpu.SemaphoreType.DMA((3,)), pltpu.SemaphoreType.DMA((3,)), pltpu.SemaphoreType.REGULAR,
            pltpu.SemaphoreType.DMA((4,)),
        ],
        compiler_params=pltpu.CompilerParams(
            collective_id=0, has_side_effects=True, vmem_limit_bytes=60 * 1024 * 1024),
    )(cotangent, speed, coeff, dirs)


def solution(mesh):
    placed = (P("gx", "gy", None), P(None, "gx", "gy", None), P(None, "gx", "gy", None), P(None, "gx", "gy"))
    return jax.shard_map(local, mesh=mesh, in_specs=placed, out_specs=P("gx", "gy", None), check_vma=False)
```

```python
import functools

import jax
import jax.numpy as jnp
from jax import lax
from jax.experimental import pallas as pl
from jax.experimental.pallas import tpu as pltpu
from jax.sharding import PartitionSpec as P

MESH = pl.DeviceIdType.MESH
F32 = jnp.float32
UNROLL = (28, 34, 16)
UI, UL, UT = (6, 7), 4, 4

BX, BY, BZ = 32, 64, 128
OX, OY = 2, 16
NX, EX, EY = BX + 2 * OX, BX + 2 * OX, BY + 2 * OY
TOP, BOT = OY, OY + BY
EXT = (EX, EY, BZ)
PARTS = {"zl": 2, "y": 4, "x": 4, "zh": 2, "c": 2}


def offsets(axes):
    found = [{}]
    for axis in axes:
        found = [dict(o, **{axis: i}) for o in found for i in range(PARTS[axis])]
    found = [o for o in found if any(o.values())]

    def distance(o):
        total = 0
        for axis, i in o.items():
            if axis in ("x", "y"):
                total += min(i, 4 - i)
            elif axis == "zh":
                total += 2 * i
            else:
                total += i
        return total

    return sorted(found, key=lambda o: -distance(o))


GROUP_A = offsets(("zl", "zh", "c"))
GROUP_B = offsets(("x", "y"))
EVERYONE = offsets(("x", "y", "zh", "zl", "c"))


def kernel(cot, speed, coeff, dirs, out, cfield, cf, vel, y4, w4, g4, qr4, y3, w3, g3, qr3, y2, w2, t1, t2, b1, sc, up_z, down_z, centre,
           signs, sums, load_sem, send, recv, ar_send, ar_recv, in_sem):
    gx, gy = lax.axis_index("gx"), lax.axis_index("gy")
    place = {"zl": gx // 4, "y": gx % 4, "x": gy // 4, "zh": (gy // 2) % 2, "c": gy % 2}

    def device(offset):
        at = {k: (place[k] + offset[k]) % PARTS[k] if offset.get(k, 0) else place[k] for k in place}
        return {"gx": at["zl"] * 4 + at["y"], "gy": at["x"] * 4 + at["zh"] * 2 + at["c"]}

    def neighbour(sx, sy):
        return {"gx": (gx + sx + 8) % 8, "gy": (gy + sy + 16) % 16}

    lane = lax.broadcasted_iota(jnp.int32, (8, BZ), 1)

    def zero_rim(ref, *lead):
        for x in (0, 1, NX - 2, NX - 1):
            ref[(*lead, x)] = jnp.zeros((EY, BZ), F32)

        def body(x, _):
            ref[(*lead, x, pl.ds(TOP - 8, 8))] = jnp.zeros((8, BZ), F32)
            ref[(*lead, x, pl.ds(BOT, 8))] = jnp.zeros((8, BZ), F32)
            return 0

        lax.fori_loop(OX, OX + BX, body, 0, unroll=8)

    inner = (pl.ds(OX, BX), pl.ds(OY, BY))
    loads = [pltpu.make_async_copy(cot, cfield.at[inner], load_sem.at[0])]
    for d in range(3):
        loads.append(pltpu.make_async_copy(speed.at[d], vel.at[(d, *inner)], load_sem.at[1 + d]))
    for d in range(3):
        loads.append(pltpu.make_async_copy(coeff.at[d], cf.at[(d, *inner)], load_sem.at[4 + d]))
    for load in loads:
        load.start()

    zero_rim(cfield)
    for d in range(3):
        zero_rim(cf, d)
    zero_rim(vel, 0)
    zero_rim(vel, 1)
    zero_rim(y4)

    barrier = pltpu.get_barrier_semaphore()
    friends = [neighbour(sx, sy) for sx in (-1, 0, 1) for sy in (-1, 0, 1) if sx or sy]
    friends += [device(o) for o in GROUP_A] + [device(o) for o in GROUP_B]
    for friend in friends:
        pl.semaphore_signal(barrier, inc=1, device_id=friend, device_id_type=MESH)

    for k in range(2):
        zero_rim(qr4, k)
    for k in range(3):
        zero_rim(qr3, k)

    signs[...] = jnp.zeros((128, 128), F32)
    for d in range(3):
        signs[pl.ds(32 * d, 32), pl.ds(0, 64)] = (1 - 2 * dirs[d]).astype(F32)
    signs[...] = signs[...].T
    for load in loads[1:4]:
        load.wait()
    columns = signs[pl.ds(0, 64), :]
    for d in range(3):
        for x in range(BX):
            k = 32 * d + x
            rows = pl.ds(OY, BY)
            vel[d, OX + x, rows] = vel[d, OX + x, rows] * columns[:, k:k + 1]
    loads[0].wait()
    for load in loads[4:]:
        load.wait()

    count = [0]
    edges = {-1: (gx > 0, gy > 0), 1: (gx < 7, gy < 15)}

    def transfer(ref, lead, source, target, sx, sy):
        k = count[0]
        count[0] += 1
        copy = pltpu.make_async_remote_copy(
            src_ref=ref.at[(*lead, *source)], dst_ref=ref.at[(*lead, *target)],
            send_sem=send.at[k], recv_sem=recv.at[k], device_id=neighbour(sx, sy), device_id_type=MESH)
        sends, receives = None, None
        if sx:
            sends, receives = edges[sx][0], edges[-sx][0]
        if sy:
            ys, yr = edges[sy][1], edges[-sy][1]
            sends = ys if sends is None else jnp.logical_and(sends, ys)
            receives = yr if receives is None else jnp.logical_and(receives, yr)
        pl.when(sends)(copy.start)
        return copy, sends, receives

    def finish(copies):
        for copy, sends, receives in copies:
            pl.when(receives)(copy.wait_recv)
            pl.when(sends)(copy.wait_send)

    XS, YS = pl.ds(OX, BX), pl.ds(OY, BY)

    def to_above(ref, lead, axis, width):
        if axis == 0:
            return transfer(ref, lead, (pl.ds(OX + BX - width, width), YS), (pl.ds(OX - width, width), YS), 1, 0)
        return transfer(ref, lead, (XS, pl.ds(BOT - width, width)), (XS, pl.ds(TOP - width, width)), 0, 1)

    def to_below(ref, lead, axis, width):
        if axis == 0:
            return transfer(ref, lead, (pl.ds(OX, width), YS), (pl.ds(OX + BX, width), YS), -1, 0)
        return transfer(ref, lead, (XS, pl.ds(TOP, width)), (XS, pl.ds(BOT, width)), 0, -1)

    def corner(ref, lead, sx, sy):
        xs, xt = (OX + BX - 1, OX - 1) if sx > 0 else (OX, OX + BX)
        ys, yt = (BOT - 1, TOP - 1) if sy > 0 else (TOP, BOT)
        return transfer(ref, lead, (pl.ds(xs, 1), pl.ds(ys, 1)), (pl.ds(xt, 1), pl.ds(yt, 1)), sx, sy)

    def swap(ref, lead):
        return [to_above(ref, lead, 0, 2), to_below(ref, lead, 0, 2), to_above(ref, lead, 1, 2),
                to_below(ref, lead, 1, 2)] + [corner(ref, lead, sx, sy) for sx in (1, -1) for sy in (1, -1)]

    def ahead_z(v):
        rows = v.shape[0]
        at = lax.broadcasted_iota(jnp.int32, (rows, BZ), 1)
        return jnp.where(at == BZ - 1, 0.0, pltpu.roll(v, BZ - 1, 1))

    def behind_z(v):
        rows = v.shape[0]
        at = lax.broadcasted_iota(jnp.int32, (rows, BZ), 1)
        return jnp.where(at == 0, 0.0, pltpu.roll(v, 1, 1))

    def stencil(src, x0, n, segments, emit, advect=True, diffuse=True, unroll=1):
        def start(r, size):
            rows = pl.ds(r, size)
            v = src[x0, rows]
            dx = v - src[x0 - 1, rows]
            parts = [v]
            if diffuse:
                parts.append(cf[0, x0 - 1, rows] * dx)
            if advect:
                parts.append(jnp.minimum(vel[0, x0 - 1, rows], 0.0) * dx)
            return tuple(parts)

        def plane(x, carry):
            done = []
            for (r, size), held in zip(segments, carry):
                rows, up, down = pl.ds(r, size), pl.ds(r + 1, size), pl.ds(r - 1, size)
                v = held[0]
                ahead = src[x + 1, rows]
                dx = ahead - v
                dyu = src[x, up] - v
                dyd = v - src[x, down]
                dz = ahead_z(v) - v
                parts = [ahead]
                dv = fv = None
                if diffuse:
                    fx = cf[0, x, rows] * dx
                    fz = cf[2, x, rows] * dz
                    dv = (fx - held[1]) + (cf[1, x, rows] * dyu - cf[1, x, down] * dyd) + (fz - behind_z(fz))
                    parts.append(fx)
                if advect:
                    u0, u1, u2 = vel[0, x, rows], vel[1, x, rows], vel[2, x, rows]
                    fv = (jnp.maximum(u0, 0.0) * dx + held[-1])
                    fv = fv + (jnp.maximum(u1, 0.0) * dyu + jnp.minimum(vel[1, x, down], 0.0) * dyd)
                    fv = fv + (jnp.maximum(u2, 0.0) * dz + behind_z(jnp.minimum(u2, 0.0) * dz))
                    parts.append(jnp.minimum(u0, 0.0) * dx)
                emit(x, rows, v, fv, dv)
                done.append(tuple(parts))
            return tuple(done)

        carry = tuple(start(r, size) for r, size in segments)
        if unroll >= n:
            for i in range(n):
                carry = plane(x0 + i, carry)
        else:
            lax.fori_loop(x0, x0 + n, plane, carry, unroll=unroll)

    def blocks(src, x0, n, px, segments, emit, advect=True, diffuse=True):
        def at(ref, lead, x, count, r, size):
            return ref[(*lead, pl.ds(x, count), pl.ds(r, size))].reshape(count * size, BZ)

        def one(x):
            for r, size in segments:
                wide = at(src, (), x - 1, px + 2, r, size)
                v = wide[size:-size]
                dx = wide[size:] - wide[:-size]
                dyu = at(src, (), x, px, r + 1, size) - v
                dyd = v - at(src, (), x, px, r - 1, size)
                dz = ahead_z(v) - v
                dv = fv = None
                if diffuse:
                    fx = at(cf, (0,), x - 1, px + 1, r, size) * dx
                    fz = at(cf, (2,), x, px, r, size) * dz
                    fy = at(cf, (1,), x, px, r, size) * dyu - at(cf, (1,), x, px, r - 1, size) * dyd
                    dv = (fx[size:] - fx[:-size]) + fy + (fz - behind_z(fz))
                if advect:
                    u0 = at(vel, (0,), x - 1, px + 1, r, size)
                    u1, u2 = at(vel, (1,), x, px, r, size), at(vel, (2,), x, px, r, size)
                    u1d = at(vel, (1,), x, px, r - 1, size)
                    fv = jnp.maximum(u0[size:], 0.0) * dx[size:] + jnp.minimum(u0[:-size], 0.0) * dx[:-size]
                    fv = fv + (jnp.maximum(u1, 0.0) * dyu + jnp.minimum(u1d, 0.0) * dyd)
                    fv = fv + (jnp.maximum(u2, 0.0) * dz + behind_z(jnp.minimum(u2, 0.0) * dz))
                emit(pl.ds(x, px), pl.ds(r, size), v, fv, dv)

        if n == px:
            one(x0)
        else:
            lax.fori_loop(0, n // px, lambda i, _: (one(x0 + i * px), 0)[1], 0)

    def shaped(x, rows, value):
        return value.reshape(x.size, rows.size, BZ) if isinstance(x, pl.Slice) else value

    def flat(value):
        return value.reshape(-1, BZ)

    WHOLE = ((OY, BY),)
    INNER = ((OY + 8, BY - 16),)
    STRIPS = ((OY, 8), (BOT - 8, 8))
    CORE = tuple((OY + 8 + 24 * i, 24) for i in range(2))
    WIDE7 = tuple((OY - 8 + 40 * i, 40) for i in range(2))
    HALVES = ((OY, BY // 2), (OY + BY // 2, BY // 2))

    def rim(src, emit, width, **kinds):
        ends = HALVES if width == 2 else WHOLE
        blocks(src, OX, width, width, ends, emit, **kinds)
        blocks(src, OX + BX - width, width, width, ends, emit, **kinds)
        blocks(src, OX + width, BX - 2 * width, 10 if width == 1 else 7, STRIPS, emit, **kinds)

    def inner_part(src, emit, width, **kinds):
        n = BX - 2 * width
        stencil(src, OX + width, n, INNER, emit, unroll=UI[width - 1], **kinds)

    def emit_y4(x, rows, v, fv, dv):
        y4[x, rows] = shaped(x, rows, 0.25 * (fv + dv))

    pl.semaphore_wait(barrier, len(friends))
    first = [to_above(cfield, (), 0, 1), to_below(cfield, (), 0, 1), to_above(cfield, (), 1, 1),
             to_below(cfield, (), 1, 1), to_above(cf, (0,), 0, 2), to_above(cf, (1,), 1, 2),
             to_above(vel, (0,), 0, 1), to_above(vel, (1,), 1, 1)]
    later = [to_above(cf, (pl.ds(1, 2),), 0, 1), to_below(cf, (pl.ds(0, 3),), 0, 1),
             to_above(cf, (0,), 1, 1), to_above(cf, (2,), 1, 1), to_below(cf, (pl.ds(0, 3),), 1, 1),
             corner(cf, (pl.ds(0, 2),), 1, 1), corner(cf, (1,), -1, 1), corner(cf, (0,), 1, -1)]
    for o in GROUP_B:
        pl.semaphore_signal(in_sem, inc=1, device_id=device(o), device_id_type=MESH)
    inner_part(cfield, emit_y4, 1)
    finish(first)
    rim(cfield, emit_y4, 1)
    moved = swap(y4, ())

    def to_w(dst):
        def emit(x, rows, v, fv, dv):
            dst[x, rows] = shaped(x, rows, -dv)
        return emit

    WIDE = ((OY - 8, BY + 16),)

    def clear_outside(ref):
        @pl.when(gx == 0)
        def _():
            ref[OX - 1] = jnp.zeros((EY, BZ), F32)

        @pl.when(gx == 7)
        def _():
            ref[OX + BX] = jnp.zeros((EY, BZ), F32)

        def rows_at(r):
            def body(x, _):
                ref[x, pl.ds(r, 8)] = jnp.zeros((8, BZ), F32)
                return 0
            lax.fori_loop(OX, OX + BX, body, 0, unroll=8)

        pl.when(gy == 0)(lambda: rows_at(TOP - 8))
        pl.when(gy == 15)(lambda: rows_at(BOT))

    def fold(values):
        return jnp.sum(values.reshape(values.shape[0] // 8, 8, BZ), axis=0)

    def moments(y, w):
        zero = jnp.zeros((8, BZ), F32)
        got = (zero,) * 4
        for r, size in HALVES:
            def plane(x, carry, r=r, size=size):
                a0, a1, a2, a3, here = carry
                rows = pl.ds(r, size)
                v = y[x, rows]
                ahead = w[x + 1, rows]
                dx = ahead - here
                dy = w[x, pl.ds(r + 1, size)] - here
                dz = ahead_z(here) - here
                energy = (cf[0, x, rows] * dx) * dx + (cf[1, x, rows] * dy) * dy + (cf[2, x, rows] * dz) * dz
                return (a0 + fold(v * v), a1 + fold(v * here), a2 + fold(here * here), a3 + fold(energy), ahead)

            got = lax.fori_loop(OX, OX + BX, plane, (*got[:4], w[OX, pl.ds(r, size)]), unroll=16)
        return got[:4]

    def send_sums(r, parts):
        row = jnp.zeros((1, BZ), F32)
        for k, part in enumerate(parts):
            total = jnp.sum(jnp.sum(part, axis=0, keepdims=True), axis=1, keepdims=True)
            row = jnp.where(lane[0:1] == k, total, row)
        sums[r, pl.ds(127, 1)] = row
        for k, o in enumerate(EVERYONE):
            pltpu.make_async_remote_copy(
                src_ref=sums.at[r, pl.ds(127, 1)], dst_ref=sums.at[r, pl.ds(k, 1)],
                send_sem=ar_send.at[r], recv_sem=ar_recv.at[r], device_id=device(o), device_id_type=MESH).start()

    def solve(r):
        pltpu.make_async_remote_copy(
            src_ref=sums.at[r, pl.ds(0, 127)], dst_ref=sums.at[r, pl.ds(0, 127)],
            send_sem=ar_send.at[r], recv_sem=ar_recv.at[r], device_id=device(EVERYONE[0]), device_id_type=MESH).wait()
        row = jnp.sum(sums[r], axis=0, keepdims=True)
        m0, k1, k2, k3 = (
            jnp.broadcast_to(jnp.sum(jnp.where(lane[0:1] == k, row, 0.0), axis=1, keepdims=True), (8, BZ))
            for k in range(4))
        h = 0.25
        alpha = m0 / (m0 + h * k1)
        rho = k1 / m0
        ss = k2 - rho * k1
        sls = k3 - 2.0 * rho * k2 + rho * (rho * k1)
        beta = (alpha * h) * (alpha * h) * (ss / m0)
        under = ss * (1.0 - beta / alpha) + h * sls
        second = jnp.where(under > 0.0, jnp.clip(ss / under, 0.0, 1.0), 0.0)
        return alpha + second * (alpha * h * rho + beta), -second * alpha * h

    def full(scalar, size):
        return jnp.concatenate([scalar] * (size // 8), axis=0)

    def held(ref, x, px, r, size, dx=0, dr=0):
        return ref[pl.ds(x + dx, px), pl.ds(r + dr, size)].reshape(px * size, BZ)

    def d_weights(x, px, r, size):
        return (held(cf.at[0], x, px, r, size), held(cf.at[0], x, px, r, size, -1),
                held(cf.at[1], x, px, r, size), held(cf.at[1], x, px, r, size, 0, -1),
                held(up_z, x, px, r, size), held(down_z, x, px, r, size), held(centre, x, px, r, size))

    def s_weights(x, px, r, size):
        return tuple(held(sc.at[k], x, px, r, size, -OX, -OY) for k in range(7))

    def seven(src, weights, emit, x, px, r, size, before, here, after):
        north, south = held(src, x, px, r, size, 0, 1), held(src, x, px, r, size, 0, -1)
        up, down = pltpu.roll(here, BZ - 1, 1), pltpu.roll(here, 1, 1)
        results = []
        for weight in weights:
            e, w, n, s, u, d, c = weight(x, px, r, size)
            results.append((e * after + w * before) + (n * north + s * south) + (u * up + d * down) - c * here)
        emit(x, px, r, size, here, *results)

    def sweep7(src, x0, n, segments, weights, emit, unroll):
        for r, size in segments:
            def plane(x, carry, r=r, size=size):
                before, here = carry
                after = held(src, x, 1, r, size, 1)
                seven(src, weights, emit, x, 1, r, size, before, here, after)
                return here, after

            lax.fori_loop(x0, x0 + n, plane, (held(src, x0, 1, r, size, -1), held(src, x0, 1, r, size)), unroll=unroll)

    def blocks7(src, x0, n, px, segments, weights, emit):
        def one(x):
            for r, size in segments:
                wide = held(src, x - 1, px + 2, r, size)
                seven(src, weights, emit, x, px, r, size, wide[:-2 * size], wide[size:-size], wide[2 * size:])

        if n == px:
            one(x0)
        else:
            lax.fori_loop(0, n // px, lambda i, _: (one(x0 + i * px), 0)[1], 0)

    def put(ref, x, px, r, size, value, dx=0, dr=0):
        ref[pl.ds(x + dx, px), pl.ds(r + dr, size)] = value.reshape(px, size, BZ)

    def advance(y, w, qr, g):
        def emit_q(x, px, r, size, v, sv):
            put(qr.at[0], x, px, r, size, sv)

        def emit_r(x, px, r, size, v, sv, dv):
            put(qr.at[1], x, px, r, size, sv)
            put(g, x, px, r, size, dv)

        def rim7(src, weights, emit):
            blocks7(src, OX, 2, 2, HALVES, weights, emit)
            blocks7(src, OX + BX - 2, 2, 2, HALVES, weights, emit)
            blocks7(src, OX + 2, BX - 4, 7, STRIPS, weights, emit)

        both = (s_weights, d_weights)
        rim7(y, (s_weights,), emit_q)
        rim7(w, both, emit_r)
        copies = swap(qr, (pl.ds(0, 2),))
        sweep7(y, OX + 2, BX - 4, CORE, (s_weights,), emit_q, UNROLL[0])
        sweep7(w, OX + 2, BX - 4, CORE, both, emit_r, UNROLL[0])
        return copies

    def laplacian7(src, dst):
        def emit(x, px, r, size, v, dv):
            put(dst, x, px, r, size, -dv)

        sweep7(src, OX - 1, BX + 2, WIDE7, (d_weights,), emit, UNROLL[1])

    def prepare_s():
        def body(x, _):
            for r, size in HALVES:
                a = [vel[d, x, pl.ds(r, size)] for d in range(3)]
                k = [0.25 * cf[d, x, pl.ds(r, size)] for d in range(3)]
                e, n, u = (0.5 * jnp.maximum(a[d], 0.0) + k[d] for d in range(3))
                w = 0.25 * cf[0, x - 1, pl.ds(r, size)] - 0.5 * jnp.minimum(vel[0, x - 1, pl.ds(r, size)], 0.0)
                s = 0.25 * cf[1, x, pl.ds(r - 1, size)] - 0.5 * jnp.minimum(vel[1, x, pl.ds(r - 1, size)], 0.0)
                d = behind_z(k[2] - 0.5 * jnp.minimum(a[2], 0.0))
                at = lax.broadcasted_iota(jnp.int32, (size, BZ), 1)
                values = (e, w, n, s, jnp.where(at == BZ - 1, 0.0, u), d, (e + w) + (n + s) + (u + d))
                for i, value in enumerate(values):
                    sc[i, x - OX, pl.ds(r - OY, size)] = value
            return 0

        lax.fori_loop(OX, OX + BX, body, 0, unroll=2)

    def prepare_d(x0, n, r, size):
        def body(x, _):
            rows = pl.ds(r, size)
            k = cf[2, x, rows]
            d = behind_z(k)
            at = lax.broadcasted_iota(jnp.int32, (size, BZ), 1)
            up_z[x, rows] = jnp.where(at == BZ - 1, 0.0, k)
            down_z[x, rows] = d
            centre[x, rows] = ((cf[0, x, rows] + cf[0, x - 1, rows]) + (cf[1, x, rows] + cf[1, x, pl.ds(r - 1, size)])
                               + (k + d))
            return 0

        lax.fori_loop(x0, x0 + n, body, 0, unroll=8 if n > 1 else 1)

    def everywhere(fn):
        def body(x, _):
            fn(x, pl.ds(OY - 8, BY + 16))
            return 0
        lax.fori_loop(0, NX, body, 0, unroll=4)

    def block(fn, unroll=4):
        def body(x, _):
            fn(x, pl.ds(OY, BY))
            return 0
        lax.fori_loop(OX, OX + BX, body, 0, unroll=unroll)

    inner_part(y4, to_w(w4), 1, advect=False)
    prepare_s()
    prepare_d(OX, BX, OY, BY)
    finish(moved)
    finish(later)
    blocks(y4, OX - 1, 2, 2, WIDE, to_w(w4), advect=False)
    blocks(y4, OX + BX - 1, 2, 2, WIDE, to_w(w4), advect=False)
    blocks(y4, OX + 1, BX - 2, 5, ((OY - 8, 16), (BOT - 8, 16)), to_w(w4), advect=False)
    clear_outside(w4)
    pl.semaphore_wait(in_sem, len(GROUP_B))
    send_sums(0, moments(y4, w4))
    moved = advance(y4, w4, qr4, g4)
    prepare_d(OX - 1, 1, OY, BY)
    prepare_d(OX + BX, 1, OY, BY)
    prepare_d(OX, BX, OY - 8, 8)
    prepare_d(OX, BX, BOT, 8)
    finish(moved)
    a4, c4 = solve(0)

    def base2(x, rows):
        size = rows.size
        a, c = full(a4, size), full(c4, size)
        qr3[2, x, rows] = (1.4 * y4[x, rows] + a * (0.6 * qr4[0, x, rows] - 0.2 * w4[x, rows])
                           + c * (0.6 * qr4[1, x, rows] + 0.2 * g4[x, rows]))

    def few(x0, n):
        for i in range(n):
            base2(x0 + i, pl.ds(OY, BY))

    def strips(i, _):
        for k in range(7):
            base2(OX + 2 + 7 * i + k, pl.ds(OY, 8))
            base2(OX + 2 + 7 * i + k, pl.ds(BOT - 8, 8))
        return 0

    few(OX, 2)
    few(OX + BX - 2, 2)
    lax.fori_loop(0, 4, strips, 0)
    moved2 = swap(qr3, (2,))

    def make_y3(x, rows):
        a, c = full(a4, rows.size), full(c4, rows.size)
        y3[x, rows] = y4[x, rows] + a * qr4[0, x, rows] + c * qr4[1, x, rows]

    everywhere(make_y3)
    laplacian7(y3, w3)
    clear_outside(w3)
    send_sums(1, moments(y3, w3))
    moved = advance(y3, w3, qr3, g3)
    lax.fori_loop(OX + 2, OX + BX - 2, lambda x, _: (base2(x, pl.ds(OY + 8, BY - 16)), 0)[1], 0, unroll=4)
    finish(moved2)
    finish(moved)
    a3, c3 = solve(1)

    def make_y2(x, rows):
        a, c = full(a3, rows.size), full(c3, rows.size)
        y2[x, rows] = qr3[2, x, rows] + a * qr3[0, x, rows] + c * qr3[1, x, rows]

    everywhere(make_y2)
    laplacian7(y2, w2)
    clear_outside(w2)
    send_sums(2, moments(y2, w2))

    def emit_t1(x, px, r, size, v, sv):
        put(t1, x, px, r, size, v + sv, -OX, -OY)

    def emit_t2(x, px, r, size, v, sv):
        put(t2, x, px, r, size, v + sv, -OX, -OY)

    sweep7(y2, OX, BX, HALVES, (s_weights,), emit_t1, UNROLL[2])
    sweep7(w2, OX, BX, HALVES, (s_weights,), emit_t2, UNROLL[2])

    def base1(x, rows):
        size = rows.size
        a, c, a_, c_ = full(a4, size), full(c4, size), full(a3, size), full(c3, size)
        total = cfield[x, rows] + 0.6 * y4[x, rows]
        total = total + a * (y4[x, rows] + 0.4 * qr4[0, x, rows] - 0.05 * w4[x, rows])
        total = total + c * (w4[x, rows] + 0.4 * qr4[1, x, rows] + 0.05 * g4[x, rows])
        total = total + a_ * (y3[x, rows] + 0.5 * qr3[0, x, rows] - 0.125 * w3[x, rows])
        total = total + c_ * (w3[x, rows] + 0.5 * qr3[1, x, rows] + 0.125 * g3[x, rows])
        b1[x - OX] = total

    block(base1)
    a2, c2 = solve(2)
    def body(x, _):
        out[x] = b1[x] + full(a2, BY) * t1[x] + full(c2, BY) * t2[x]
        return 0

    lax.fori_loop(0, BX, body, 0, unroll=8)


COPIES = 80


def local(cotangent, speed, coeff, dirs):
    ext = pltpu.VMEM(EXT, F32)
    plain = pltpu.VMEM((BX, BY, BZ), F32)

    def stack(n):
        return pltpu.VMEM((n, *EXT), F32)

    anywhere = pl.BlockSpec(memory_space=pl.ANY)
    return pl.pallas_call(
        kernel,
        name="adjoint_step",
        out_shape=jax.ShapeDtypeStruct((BX, BY, BZ), F32),
        in_specs=[anywhere, anywhere, anywhere, pl.BlockSpec(memory_space=pltpu.VMEM)],
        out_specs=pl.BlockSpec(memory_space=pltpu.VMEM),
        scratch_shapes=[
            ext, stack(3), stack(3), ext, ext, ext, stack(2), ext, ext, ext, stack(3), ext, ext,
            plain, plain, plain, pltpu.VMEM((7, BX, BY, BZ), F32), ext, ext, ext, pltpu.VMEM((128, 128), F32), pltpu.VMEM((3, 128, BZ), F32),
            pltpu.SemaphoreType.DMA((7,)), pltpu.SemaphoreType.DMA((COPIES,)), pltpu.SemaphoreType.DMA((COPIES,)),
            pltpu.SemaphoreType.DMA((3,)), pltpu.SemaphoreType.DMA((3,)), pltpu.SemaphoreType.REGULAR,
        ],
        compiler_params=pltpu.CompilerParams(
            collective_id=0, has_side_effects=True, vmem_limit_bytes=57 * 1024 * 1024),
    )(cotangent, speed, coeff, dirs)


def solution(mesh):
    placed = (P("gx", "gy", None), P(None, "gx", "gy", None), P(None, "gx", "gy", None), P(None, "gx", "gy"))
    return jax.shard_map(local, mesh=mesh, in_specs=placed, out_specs=P("gx", "gy", None), check_vma=False)
```

```python
import functools

import jax
import jax.numpy as jnp
from jax import lax
from jax.experimental import pallas as pl
from jax.experimental.pallas import tpu as pltpu
from jax.sharding import PartitionSpec as P

MESH = pl.DeviceIdType.MESH
F32 = jnp.float32
UNROLL = (28, 34, 16)
UI, UL, UT = (6, 7), 4, 4

BX, BY, BZ = 32, 64, 128
OX, OY = 2, 16
NX, EX, EY = BX + 2 * OX, BX + 2 * OX, BY + 2 * OY
TOP, BOT = OY, OY + BY
EXT = (EX, EY, BZ)
PARTS = {"zl": 2, "y": 4, "x": 4, "zh": 2, "c": 2}


def offsets(axes):
    found = [{}]
    for axis in axes:
        found = [dict(o, **{axis: i}) for o in found for i in range(PARTS[axis])]
    found = [o for o in found if any(o.values())]

    def distance(o):
        total = 0
        for axis, i in o.items():
            if axis in ("x", "y"):
                total += min(i, 4 - i)
            elif axis == "zh":
                total += 2 * i
            else:
                total += i
        return total

    return sorted(found, key=lambda o: -distance(o))


GROUP_A = offsets(("zl", "zh", "c"))
GROUP_B = offsets(("x", "y"))
EVERYONE = offsets(("x", "y", "zh", "zl", "c"))


def kernel(cot, speed, coeff, dirs, out, cfield, cf, vel, y4, w4, g4, qr4, y3, w3, g3, qr3, y2, w2, t1, t2, b1, sc, up_z, down_z, centre,
           ways, signs, sums, load_sem, send, recv, ar_send, ar_recv, in_sem):
    gx, gy = lax.axis_index("gx"), lax.axis_index("gy")
    place = {"zl": gx // 4, "y": gx % 4, "x": gy // 4, "zh": (gy // 2) % 2, "c": gy % 2}

    def device(offset):
        at = {k: (place[k] + offset[k]) % PARTS[k] if offset.get(k, 0) else place[k] for k in place}
        return {"gx": at["zl"] * 4 + at["y"], "gy": at["x"] * 4 + at["zh"] * 2 + at["c"]}

    def neighbour(sx, sy):
        return {"gx": (gx + sx + 8) % 8, "gy": (gy + sy + 16) % 16}

    lane = lax.broadcasted_iota(jnp.int32, (8, BZ), 1)

    def zero_rim(ref, *lead):
        for x in (0, 1, NX - 2, NX - 1):
            ref[(*lead, x)] = jnp.zeros((EY, BZ), F32)

        def body(x, _):
            ref[(*lead, x, pl.ds(TOP - 8, 8))] = jnp.zeros((8, BZ), F32)
            ref[(*lead, x, pl.ds(BOT, 8))] = jnp.zeros((8, BZ), F32)
            return 0

        lax.fori_loop(OX, OX + BX, body, 0, unroll=8)

    inner = (pl.ds(OX, BX), pl.ds(OY, BY))
    loads = [pltpu.make_async_copy(cot, cfield.at[inner], load_sem.at[0])]
    for d in range(3):
        loads.append(pltpu.make_async_copy(speed.at[d], vel.at[(d, *inner)], load_sem.at[1 + d]))
    for d in range(3):
        loads.append(pltpu.make_async_copy(coeff.at[d], cf.at[(d, *inner)], load_sem.at[4 + d]))
    loads.append(pltpu.make_async_copy(dirs, ways, load_sem.at[7]))
    for k in (7, 1, 2, 0, 4, 5, 6, 3):
        loads[k].start()

    zero_rim(cfield)
    for d in range(3):
        zero_rim(cf, d)
    zero_rim(vel, 0)
    zero_rim(vel, 1)
    zero_rim(y4)

    barrier = pltpu.get_barrier_semaphore()
    friends = [neighbour(sx, sy) for sx in (-1, 0, 1) for sy in (-1, 0, 1) if sx or sy]
    friends += [device(o) for o in GROUP_A] + [device(o) for o in GROUP_B]
    for friend in friends:
        pl.semaphore_signal(barrier, inc=1, device_id=friend, device_id_type=MESH)

    for k in range(2):
        zero_rim(qr4, k)
    for k in range(3):
        zero_rim(qr3, k)

    signs[...] = jnp.zeros((128, 128), F32)
    loads[7].wait()
    for d in range(3):
        signs[pl.ds(32 * d, 32), pl.ds(0, 64)] = (1 - 2 * ways[d]).astype(F32)
    signs[...] = signs[...].T

    def sign(d, x, r, size):
        rows, k = pl.ds(OY + r, size), 32 * d + x
        vel[d, OX + x, rows] = vel[d, OX + x, rows] * signs[pl.ds(r, size), k:k + 1]

    loads[1].wait()
    sign(0, BX - 1, 0, BY)
    loads[2].wait()
    for x in range(BX):
        sign(1, x, BY - 8, 8)
    for k in (0, 4, 5, 6):
        loads[k].wait()

    count = [0]
    edges = {-1: (gx > 0, gy > 0), 1: (gx < 7, gy < 15)}

    def transfer(ref, lead, source, target, sx, sy):
        k = count[0]
        count[0] += 1
        copy = pltpu.make_async_remote_copy(
            src_ref=ref.at[(*lead, *source)], dst_ref=ref.at[(*lead, *target)],
            send_sem=send.at[k], recv_sem=recv.at[k], device_id=neighbour(sx, sy), device_id_type=MESH)
        sends, receives = None, None
        if sx:
            sends, receives = edges[sx][0], edges[-sx][0]
        if sy:
            ys, yr = edges[sy][1], edges[-sy][1]
            sends = ys if sends is None else jnp.logical_and(sends, ys)
            receives = yr if receives is None else jnp.logical_and(receives, yr)
        pl.when(sends)(copy.start)
        return copy, sends, receives

    def finish(copies):
        for copy, sends, receives in copies:
            pl.when(receives)(copy.wait_recv)
            pl.when(sends)(copy.wait_send)

    XS, YS = pl.ds(OX, BX), pl.ds(OY, BY)

    def to_above(ref, lead, axis, width):
        if axis == 0:
            return transfer(ref, lead, (pl.ds(OX + BX - width, width), YS), (pl.ds(OX - width, width), YS), 1, 0)
        return transfer(ref, lead, (XS, pl.ds(BOT - width, width)), (XS, pl.ds(TOP - width, width)), 0, 1)

    def to_below(ref, lead, axis, width):
        if axis == 0:
            return transfer(ref, lead, (pl.ds(OX, width), YS), (pl.ds(OX + BX, width), YS), -1, 0)
        return transfer(ref, lead, (XS, pl.ds(TOP, width)), (XS, pl.ds(BOT, width)), 0, -1)

    def corner(ref, lead, sx, sy):
        xs, xt = (OX + BX - 1, OX - 1) if sx > 0 else (OX, OX + BX)
        ys, yt = (BOT - 1, TOP - 1) if sy > 0 else (TOP, BOT)
        return transfer(ref, lead, (pl.ds(xs, 1), pl.ds(ys, 1)), (pl.ds(xt, 1), pl.ds(yt, 1)), sx, sy)

    def swap(ref, lead):
        return [to_above(ref, lead, 0, 2), to_below(ref, lead, 0, 2), to_above(ref, lead, 1, 2),
                to_below(ref, lead, 1, 2)] + [corner(ref, lead, sx, sy) for sx in (1, -1) for sy in (1, -1)]

    def ahead_z(v):
        rows = v.shape[0]
        at = lax.broadcasted_iota(jnp.int32, (rows, BZ), 1)
        return jnp.where(at == BZ - 1, 0.0, pltpu.roll(v, BZ - 1, 1))

    def behind_z(v):
        rows = v.shape[0]
        at = lax.broadcasted_iota(jnp.int32, (rows, BZ), 1)
        return jnp.where(at == 0, 0.0, pltpu.roll(v, 1, 1))

    def stencil(src, x0, n, segments, emit, advect=True, diffuse=True, unroll=1):
        def start(r, size):
            rows = pl.ds(r, size)
            v = src[x0, rows]
            dx = v - src[x0 - 1, rows]
            parts = [v]
            if diffuse:
                parts.append(cf[0, x0 - 1, rows] * dx)
            if advect:
                parts.append(jnp.minimum(vel[0, x0 - 1, rows], 0.0) * dx)
            return tuple(parts)

        def plane(x, carry):
            done = []
            for (r, size), held in zip(segments, carry):
                rows, up, down = pl.ds(r, size), pl.ds(r + 1, size), pl.ds(r - 1, size)
                v = held[0]
                ahead = src[x + 1, rows]
                dx = ahead - v
                dyu = src[x, up] - v
                dyd = v - src[x, down]
                dz = ahead_z(v) - v
                parts = [ahead]
                dv = fv = None
                if diffuse:
                    fx = cf[0, x, rows] * dx
                    fz = cf[2, x, rows] * dz
                    dv = (fx - held[1]) + (cf[1, x, rows] * dyu - cf[1, x, down] * dyd) + (fz - behind_z(fz))
                    parts.append(fx)
                if advect:
                    u0, u1, u2 = vel[0, x, rows], vel[1, x, rows], vel[2, x, rows]
                    fv = (jnp.maximum(u0, 0.0) * dx + held[-1])
                    fv = fv + (jnp.maximum(u1, 0.0) * dyu + jnp.minimum(vel[1, x, down], 0.0) * dyd)
                    fv = fv + (jnp.maximum(u2, 0.0) * dz + behind_z(jnp.minimum(u2, 0.0) * dz))
                    parts.append(jnp.minimum(u0, 0.0) * dx)
                emit(x, rows, v, fv, dv)
                done.append(tuple(parts))
            return tuple(done)

        carry = tuple(start(r, size) for r, size in segments)
        if unroll >= n:
            for i in range(n):
                carry = plane(x0 + i, carry)
        else:
            lax.fori_loop(x0, x0 + n, plane, carry, unroll=unroll)

    def blocks(src, x0, n, px, segments, emit, advect=True, diffuse=True):
        def at(ref, lead, x, count, r, size):
            return ref[(*lead, pl.ds(x, count), pl.ds(r, size))].reshape(count * size, BZ)

        def one(x):
            for r, size in segments:
                wide = at(src, (), x - 1, px + 2, r, size)
                v = wide[size:-size]
                dx = wide[size:] - wide[:-size]
                dyu = at(src, (), x, px, r + 1, size) - v
                dyd = v - at(src, (), x, px, r - 1, size)
                dz = ahead_z(v) - v
                dv = fv = None
                if diffuse:
                    fx = at(cf, (0,), x - 1, px + 1, r, size) * dx
                    fz = at(cf, (2,), x, px, r, size) * dz
                    fy = at(cf, (1,), x, px, r, size) * dyu - at(cf, (1,), x, px, r - 1, size) * dyd
                    dv = (fx[size:] - fx[:-size]) + fy + (fz - behind_z(fz))
                if advect:
                    u0 = at(vel, (0,), x - 1, px + 1, r, size)
                    u1, u2 = at(vel, (1,), x, px, r, size), at(vel, (2,), x, px, r, size)
                    u1d = at(vel, (1,), x, px, r - 1, size)
                    fv = jnp.maximum(u0[size:], 0.0) * dx[size:] + jnp.minimum(u0[:-size], 0.0) * dx[:-size]
                    fv = fv + (jnp.maximum(u1, 0.0) * dyu + jnp.minimum(u1d, 0.0) * dyd)
                    fv = fv + (jnp.maximum(u2, 0.0) * dz + behind_z(jnp.minimum(u2, 0.0) * dz))
                emit(pl.ds(x, px), pl.ds(r, size), v, fv, dv)

        if n == px:
            one(x0)
        else:
            lax.fori_loop(0, n // px, lambda i, _: (one(x0 + i * px), 0)[1], 0)

    def shaped(x, rows, value):
        return value.reshape(x.size, rows.size, BZ) if isinstance(x, pl.Slice) else value

    def flat(value):
        return value.reshape(-1, BZ)

    WHOLE = ((OY, BY),)
    INNER = ((OY + 8, BY - 16),)
    STRIPS = ((OY, 8), (BOT - 8, 8))
    CORE = tuple((OY + 8 + 24 * i, 24) for i in range(2))
    WIDE7 = tuple((OY - 8 + 40 * i, 40) for i in range(2))
    HALVES = ((OY, BY // 2), (OY + BY // 2, BY // 2))

    def rim(src, emit, width, **kinds):
        ends = HALVES if width == 2 else WHOLE
        blocks(src, OX, width, width, ends, emit, **kinds)
        blocks(src, OX + BX - width, width, width, ends, emit, **kinds)
        blocks(src, OX + width, BX - 2 * width, 10 if width == 1 else 7, STRIPS, emit, **kinds)

    def inner_part(src, emit, width, **kinds):
        n = BX - 2 * width
        stencil(src, OX + width, n, INNER, emit, unroll=UI[width - 1], **kinds)

    def emit_y4(x, rows, v, fv, dv):
        y4[x, rows] = shaped(x, rows, 0.25 * (fv + dv))

    pl.semaphore_wait(barrier, len(friends))
    first = [to_above(cfield, (), 0, 1), to_below(cfield, (), 0, 1), to_above(cfield, (), 1, 1),
             to_below(cfield, (), 1, 1), to_above(cf, (0,), 0, 2), to_above(cf, (1,), 1, 2),
             to_above(vel, (0,), 0, 1), to_above(vel, (1,), 1, 1)]
    later = [to_above(cf, (pl.ds(1, 2),), 0, 1), to_below(cf, (pl.ds(0, 3),), 0, 1),
             to_above(cf, (0,), 1, 1), to_above(cf, (2,), 1, 1), to_below(cf, (pl.ds(0, 3),), 1, 1),
             corner(cf, (pl.ds(0, 2),), 1, 1), corner(cf, (1,), -1, 1), corner(cf, (0,), 1, -1)]
    for o in GROUP_B:
        pl.semaphore_signal(in_sem, inc=1, device_id=device(o), device_id_type=MESH)
    loads[3].wait()
    for x in range(BX):
        if x < BX - 1:
            sign(0, x, 0, BY)
        sign(1, x, 0, BY - 8)
        sign(2, x, 0, BY)
    inner_part(cfield, emit_y4, 1)
    finish(first)
    rim(cfield, emit_y4, 1)
    moved = swap(y4, ())

    def to_w(dst):
        def emit(x, rows, v, fv, dv):
            dst[x, rows] = shaped(x, rows, -dv)
        return emit

    WIDE = ((OY - 8, BY + 16),)

    def clear_outside(ref):
        @pl.when(gx == 0)
        def _():
            ref[OX - 1] = jnp.zeros((EY, BZ), F32)

        @pl.when(gx == 7)
        def _():
            ref[OX + BX] = jnp.zeros((EY, BZ), F32)

        def rows_at(r):
            def body(x, _):
                ref[x, pl.ds(r, 8)] = jnp.zeros((8, BZ), F32)
                return 0
            lax.fori_loop(OX, OX + BX, body, 0, unroll=8)

        pl.when(gy == 0)(lambda: rows_at(TOP - 8))
        pl.when(gy == 15)(lambda: rows_at(BOT))

    def fold(values):
        return jnp.sum(values.reshape(values.shape[0] // 8, 8, BZ), axis=0)

    def moments(y, w):
        zero = jnp.zeros((8, BZ), F32)
        got = (zero,) * 4
        for r, size in HALVES:
            def plane(x, carry, r=r, size=size):
                a0, a1, a2, a3, here = carry
                rows = pl.ds(r, size)
                v = y[x, rows]
                ahead = w[x + 1, rows]
                dx = ahead - here
                dy = w[x, pl.ds(r + 1, size)] - here
                dz = ahead_z(here) - here
                energy = (cf[0, x, rows] * dx) * dx + (cf[1, x, rows] * dy) * dy + (cf[2, x, rows] * dz) * dz
                return (a0 + fold(v * v), a1 + fold(v * here), a2 + fold(here * here), a3 + fold(energy), ahead)

            got = lax.fori_loop(OX, OX + BX, plane, (*got[:4], w[OX, pl.ds(r, size)]), unroll=16)
        return got[:4]

    def send_sums(r, parts):
        row = jnp.zeros((1, BZ), F32)
        for k, part in enumerate(parts):
            total = jnp.sum(jnp.sum(part, axis=0, keepdims=True), axis=1, keepdims=True)
            row = jnp.where(lane[0:1] == k, total, row)
        sums[r, pl.ds(127, 1)] = row
        for k, o in enumerate(EVERYONE):
            pltpu.make_async_remote_copy(
                src_ref=sums.at[r, pl.ds(127, 1)], dst_ref=sums.at[r, pl.ds(k, 1)],
                send_sem=ar_send.at[r], recv_sem=ar_recv.at[r], device_id=device(o), device_id_type=MESH).start()

    def solve(r):
        pltpu.make_async_remote_copy(
            src_ref=sums.at[r, pl.ds(0, 127)], dst_ref=sums.at[r, pl.ds(0, 127)],
            send_sem=ar_send.at[r], recv_sem=ar_recv.at[r], device_id=device(EVERYONE[0]), device_id_type=MESH).wait()
        row = jnp.sum(sums[r], axis=0, keepdims=True)
        m0, k1, k2, k3 = (
            jnp.broadcast_to(jnp.sum(jnp.where(lane[0:1] == k, row, 0.0), axis=1, keepdims=True), (8, BZ))
            for k in range(4))
        h = 0.25
        alpha = m0 / (m0 + h * k1)
        rho = k1 / m0
        ss = k2 - rho * k1
        sls = k3 - 2.0 * rho * k2 + rho * (rho * k1)
        beta = (alpha * h) * (alpha * h) * (ss / m0)
        under = ss * (1.0 - beta / alpha) + h * sls
        second = jnp.where(under > 0.0, jnp.clip(ss / under, 0.0, 1.0), 0.0)
        return alpha + second * (alpha * h * rho + beta), -second * alpha * h

    def full(scalar, size):
        return jnp.concatenate([scalar] * (size // 8), axis=0)

    def held(ref, x, px, r, size, dx=0, dr=0):
        return ref[pl.ds(x + dx, px), pl.ds(r + dr, size)].reshape(px * size, BZ)

    def d_weights(x, px, r, size):
        return (held(cf.at[0], x, px, r, size), held(cf.at[0], x, px, r, size, -1),
                held(cf.at[1], x, px, r, size), held(cf.at[1], x, px, r, size, 0, -1),
                held(up_z, x, px, r, size), held(down_z, x, px, r, size), held(centre, x, px, r, size))

    def s_weights(x, px, r, size):
        return tuple(held(sc.at[k], x, px, r, size, -OX, -OY) for k in range(7))

    def seven(src, weights, emit, x, px, r, size, before, here, after):
        north, south = held(src, x, px, r, size, 0, 1), held(src, x, px, r, size, 0, -1)
        up, down = pltpu.roll(here, BZ - 1, 1), pltpu.roll(here, 1, 1)
        results = []
        for weight in weights:
            e, w, n, s, u, d, c = weight(x, px, r, size)
            results.append((e * after + w * before) + (n * north + s * south) + (u * up + d * down) - c * here)
        emit(x, px, r, size, here, *results)

    def sweep7(src, x0, n, segments, weights, emit, unroll):
        for r, size in segments:
            def plane(x, carry, r=r, size=size):
                before, here = carry
                after = held(src, x, 1, r, size, 1)
                seven(src, weights, emit, x, 1, r, size, before, here, after)
                return here, after

            lax.fori_loop(x0, x0 + n, plane, (held(src, x0, 1, r, size, -1), held(src, x0, 1, r, size)), unroll=unroll)

    def blocks7(src, x0, n, px, segments, weights, emit):
        def one(x):
            for r, size in segments:
                wide = held(src, x - 1, px + 2, r, size)
                seven(src, weights, emit, x, px, r, size, wide[:-2 * size], wide[size:-size], wide[2 * size:])

        if n == px:
            one(x0)
        else:
            lax.fori_loop(0, n // px, lambda i, _: (one(x0 + i * px), 0)[1], 0)

    def put(ref, x, px, r, size, value, dx=0, dr=0):
        ref[pl.ds(x + dx, px), pl.ds(r + dr, size)] = value.reshape(px, size, BZ)

    def advance(y, w, qr, g, r):
        def emit_q(x, px, r, size, v, sv):
            put(qr.at[0], x, px, r, size, sv)

        def emit_r(x, px, r, size, v, sv, dv):
            put(qr.at[1], x, px, r, size, sv)
            put(g, x, px, r, size, dv)

        def rim7(src, weights, emit):
            blocks7(src, OX, 2, 2, HALVES, weights, emit)
            blocks7(src, OX + BX - 2, 2, 2, HALVES, weights, emit)
            blocks7(src, OX + 2, BX - 4, 7, STRIPS, weights, emit)

        both = (s_weights, d_weights)
        rim7(y, (s_weights,), emit_q)
        copies = swap(qr, (0,))
        send_sums(r, moments(y, w))
        rim7(w, both, emit_r)
        copies += swap(qr, (1,))
        sweep7(y, OX + 2, BX - 4, CORE, (s_weights,), emit_q, UNROLL[0])
        sweep7(w, OX + 2, BX - 4, CORE, both, emit_r, UNROLL[0])
        return copies

    def laplacian7(src, dst):
        def emit(x, px, r, size, v, dv):
            put(dst, x, px, r, size, -dv)

        sweep7(src, OX - 1, BX + 2, WIDE7, (d_weights,), emit, UNROLL[1])

    def prepare_s():
        def body(x, _):
            for r, size in HALVES:
                a = [vel[d, x, pl.ds(r, size)] for d in range(3)]
                k = [0.25 * cf[d, x, pl.ds(r, size)] for d in range(3)]
                e, n, u = (0.5 * jnp.maximum(a[d], 0.0) + k[d] for d in range(3))
                w = 0.25 * cf[0, x - 1, pl.ds(r, size)] - 0.5 * jnp.minimum(vel[0, x - 1, pl.ds(r, size)], 0.0)
                s = 0.25 * cf[1, x, pl.ds(r - 1, size)] - 0.5 * jnp.minimum(vel[1, x, pl.ds(r - 1, size)], 0.0)
                d = behind_z(k[2] - 0.5 * jnp.minimum(a[2], 0.0))
                at = lax.broadcasted_iota(jnp.int32, (size, BZ), 1)
                values = (e, w, n, s, jnp.where(at == BZ - 1, 0.0, u), d, (e + w) + (n + s) + (u + d))
                for i, value in enumerate(values):
                    sc[i, x - OX, pl.ds(r - OY, size)] = value
            return 0

        lax.fori_loop(OX, OX + BX, body, 0, unroll=2)

    def prepare_d(x0, n, r, size):
        def body(x, _):
            rows = pl.ds(r, size)
            k = cf[2, x, rows]
            d = behind_z(k)
            at = lax.broadcasted_iota(jnp.int32, (size, BZ), 1)
            up_z[x, rows] = jnp.where(at == BZ - 1, 0.0, k)
            down_z[x, rows] = d
            centre[x, rows] = ((cf[0, x, rows] + cf[0, x - 1, rows]) + (cf[1, x, rows] + cf[1, x, pl.ds(r - 1, size)])
                               + (k + d))
            return 0

        lax.fori_loop(x0, x0 + n, body, 0, unroll=8 if n > 1 else 1)

    def everywhere(fn):
        def body(x, _):
            fn(x, pl.ds(OY - 8, BY + 16))
            return 0
        lax.fori_loop(0, NX, body, 0, unroll=4)

    def block(fn, unroll=4):
        def body(x, _):
            fn(x, pl.ds(OY, BY))
            return 0
        lax.fori_loop(OX, OX + BX, body, 0, unroll=unroll)

    inner_part(y4, to_w(w4), 1, advect=False)
    prepare_s()
    prepare_d(OX, BX, OY, BY)
    finish(moved)
    finish(later)
    blocks(y4, OX - 1, 2, 2, WIDE, to_w(w4), advect=False)
    blocks(y4, OX + BX - 1, 2, 2, WIDE, to_w(w4), advect=False)
    blocks(y4, OX + 1, BX - 2, 5, ((OY - 8, 16), (BOT - 8, 16)), to_w(w4), advect=False)
    clear_outside(w4)
    pl.semaphore_wait(in_sem, len(GROUP_B))
    moved = advance(y4, w4, qr4, g4, 0)
    prepare_d(OX - 1, 1, OY, BY)
    prepare_d(OX + BX, 1, OY, BY)
    prepare_d(OX, BX, OY - 8, 8)
    prepare_d(OX, BX, BOT, 8)
    finish(moved)
    a4, c4 = solve(0)

    def base2(x, rows):
        size = rows.size
        a, c = full(a4, size), full(c4, size)
        qr3[2, x, rows] = (1.4 * y4[x, rows] + a * (0.6 * qr4[0, x, rows] - 0.2 * w4[x, rows])
                           + c * (0.6 * qr4[1, x, rows] + 0.2 * g4[x, rows]))

    def few(x0, n):
        for i in range(n):
            base2(x0 + i, pl.ds(OY, BY))

    def strips(i, _):
        for k in range(7):
            base2(OX + 2 + 7 * i + k, pl.ds(OY, 8))
            base2(OX + 2 + 7 * i + k, pl.ds(BOT - 8, 8))
        return 0

    few(OX, 2)
    few(OX + BX - 2, 2)
    lax.fori_loop(0, 4, strips, 0)
    moved2 = swap(qr3, (2,))

    def make_y3(x, rows):
        a, c = full(a4, rows.size), full(c4, rows.size)
        y3[x, rows] = y4[x, rows] + a * qr4[0, x, rows] + c * qr4[1, x, rows]

    everywhere(make_y3)
    laplacian7(y3, w3)
    clear_outside(w3)
    moved = advance(y3, w3, qr3, g3, 1)
    lax.fori_loop(OX + 2, OX + BX - 2, lambda x, _: (base2(x, pl.ds(OY + 8, BY - 16)), 0)[1], 0, unroll=4)
    finish(moved2)
    finish(moved)
    a3, c3 = solve(1)

    def make_y2(x, rows):
        a, c = full(a3, rows.size), full(c3, rows.size)
        y2[x, rows] = qr3[2, x, rows] + a * qr3[0, x, rows] + c * qr3[1, x, rows]

    everywhere(make_y2)
    laplacian7(y2, w2)
    clear_outside(w2)
    send_sums(2, moments(y2, w2))

    def emit_t1(x, px, r, size, v, sv):
        put(t1, x, px, r, size, v + sv, -OX, -OY)

    def emit_t2(x, px, r, size, v, sv):
        put(t2, x, px, r, size, v + sv, -OX, -OY)

    sweep7(y2, OX, BX, HALVES, (s_weights,), emit_t1, UNROLL[2])
    sweep7(w2, OX, BX, HALVES, (s_weights,), emit_t2, UNROLL[2])

    def base1(x, rows):
        size = rows.size
        a, c, a_, c_ = full(a4, size), full(c4, size), full(a3, size), full(c3, size)
        total = cfield[x, rows] + 0.6 * y4[x, rows]
        total = total + a * (y4[x, rows] + 0.4 * qr4[0, x, rows] - 0.05 * w4[x, rows])
        total = total + c * (w4[x, rows] + 0.4 * qr4[1, x, rows] + 0.05 * g4[x, rows])
        total = total + a_ * (y3[x, rows] + 0.5 * qr3[0, x, rows] - 0.125 * w3[x, rows])
        total = total + c_ * (w3[x, rows] + 0.5 * qr3[1, x, rows] + 0.125 * g3[x, rows])
        b1[x - OX] = total

    block(base1)
    a2, c2 = solve(2)
    def body(x, _):
        out[x] = b1[x] + full(a2, BY) * t1[x] + full(c2, BY) * t2[x]
        return 0

    lax.fori_loop(0, BX, body, 0, unroll=8)


COPIES = 80


def local(cotangent, speed, coeff, dirs):
    ext = pltpu.VMEM(EXT, F32)
    plain = pltpu.VMEM((BX, BY, BZ), F32)

    def stack(n):
        return pltpu.VMEM((n, *EXT), F32)

    anywhere = pl.BlockSpec(memory_space=pl.ANY)
    return pl.pallas_call(
        kernel,
        name="adjoint_step",
        out_shape=jax.ShapeDtypeStruct((BX, BY, BZ), F32),
        in_specs=[anywhere] * 4,
        out_specs=pl.BlockSpec(memory_space=pltpu.VMEM),
        scratch_shapes=[
            ext, stack(3), stack(3), ext, ext, ext, stack(2), ext, ext, ext, stack(3), ext, ext,
            plain, plain, plain, pltpu.VMEM((7, BX, BY, BZ), F32), ext, ext, ext, pltpu.VMEM((3, BX, BY), jnp.int32), pltpu.VMEM((128, 128), F32), pltpu.VMEM((3, 128, BZ), F32),
            pltpu.SemaphoreType.DMA((8,)), pltpu.SemaphoreType.DMA((COPIES,)), pltpu.SemaphoreType.DMA((COPIES,)),
            pltpu.SemaphoreType.DMA((3,)), pltpu.SemaphoreType.DMA((3,)), pltpu.SemaphoreType.REGULAR,
        ],
        compiler_params=pltpu.CompilerParams(
            collective_id=0, has_side_effects=True, vmem_limit_bytes=57 * 1024 * 1024),
    )(cotangent, speed, coeff, dirs)


def solution(mesh):
    placed = (P("gx", "gy", None), P(None, "gx", "gy", None), P(None, "gx", "gy", None), P(None, "gx", "gy"))
    return jax.shard_map(local, mesh=mesh, in_specs=placed, out_specs=P("gx", "gy", None), check_vma=False)
```

```python
import functools

import jax
import jax.numpy as jnp
from jax import lax
from jax.experimental import pallas as pl
from jax.experimental.pallas import tpu as pltpu
from jax.sharding import PartitionSpec as P

MESH = pl.DeviceIdType.MESH
F32 = jnp.float32
UNROLL = (28, 34, 16)
UI, UL, UT = (6, 7), 4, 4

BX, BY, BZ = 32, 64, 128
OX, OY = 2, 16
NX, EX, EY = BX + 2 * OX, BX + 2 * OX, BY + 2 * OY
TOP, BOT = OY, OY + BY
EXT = (EX, EY, BZ)
PARTS = {"zl": 2, "y": 4, "x": 4, "zh": 2, "c": 2}


def offsets(axes):
    found = [{}]
    for axis in axes:
        found = [dict(o, **{axis: i}) for o in found for i in range(PARTS[axis])]
    found = [o for o in found if any(o.values())]

    def distance(o):
        total = 0
        for axis, i in o.items():
            if axis in ("x", "y"):
                total += min(i, 4 - i)
            elif axis == "zh":
                total += 2 * i
            else:
                total += i
        return total

    return sorted(found, key=lambda o: -distance(o))


GROUP_A = offsets(("zl", "zh", "c"))
GROUP_B = offsets(("x", "y"))
EVERYONE = offsets(("x", "y", "zh", "zl", "c"))


def kernel(cot, speed, coeff, dirs, out, cfield, cf, vel, y4, w4, g4, qr4, y3, w3, g3, qr3, y2, w2, t1, t2, b1, sc, up_z, down_z, centre,
           ways, signs, sums, load_sem, send, recv, ar_send, ar_recv, in_sem):
    gx, gy = lax.axis_index("gx"), lax.axis_index("gy")
    place = {"zl": gx // 4, "y": gx % 4, "x": gy // 4, "zh": (gy // 2) % 2, "c": gy % 2}

    def device(offset):
        at = {k: (place[k] + offset[k]) % PARTS[k] if offset.get(k, 0) else place[k] for k in place}
        return {"gx": at["zl"] * 4 + at["y"], "gy": at["x"] * 4 + at["zh"] * 2 + at["c"]}

    def neighbour(sx, sy):
        return {"gx": (gx + sx + 8) % 8, "gy": (gy + sy + 16) % 16}

    lane = lax.broadcasted_iota(jnp.int32, (8, BZ), 1)

    def zero_rim(ref, *lead):
        for x in (0, 1, NX - 2, NX - 1):
            ref[(*lead, x)] = jnp.zeros((EY, BZ), F32)

        def body(x, _):
            ref[(*lead, x, pl.ds(TOP - 8, 8))] = jnp.zeros((8, BZ), F32)
            ref[(*lead, x, pl.ds(BOT, 8))] = jnp.zeros((8, BZ), F32)
            return 0

        lax.fori_loop(OX, OX + BX, body, 0, unroll=8)

    inner = (pl.ds(OX, BX), pl.ds(OY, BY))
    loads = [pltpu.make_async_copy(cot, cfield.at[inner], load_sem.at[0])]
    for d in range(3):
        loads.append(pltpu.make_async_copy(speed.at[d], vel.at[(d, *inner)], load_sem.at[1 + d]))
    for d in range(3):
        loads.append(pltpu.make_async_copy(coeff.at[d], cf.at[(d, *inner)], load_sem.at[4 + d]))
    loads.append(pltpu.make_async_copy(dirs, ways, load_sem.at[7]))
    for k in (7, 1, 2, 0, 4, 5, 6, 3):
        loads[k].start()

    zero_rim(cfield)
    for d in range(3):
        zero_rim(cf, d)
    zero_rim(vel, 0)
    zero_rim(vel, 1)
    zero_rim(y4)

    barrier = pltpu.get_barrier_semaphore()
    friends = [neighbour(sx, sy) for sx in (-1, 0, 1) for sy in (-1, 0, 1) if sx or sy]
    friends += [device(o) for o in GROUP_A] + [device(o) for o in GROUP_B]
    for friend in friends:
        pl.semaphore_signal(barrier, inc=1, device_id=friend, device_id_type=MESH)

    for k in range(2):
        zero_rim(qr4, k)
    for k in range(3):
        zero_rim(qr3, k)

    signs[...] = jnp.zeros((128, 128), F32)
    loads[7].wait()
    for d in range(3):
        signs[pl.ds(32 * d, 32), pl.ds(0, 64)] = (1 - 2 * ways[d]).astype(F32)
    signs[...] = signs[...].T

    def sign(d, x, r, size):
        rows, k = pl.ds(OY + r, size), 32 * d + x
        vel[d, OX + x, rows] = vel[d, OX + x, rows] * signs[pl.ds(r, size), k:k + 1]

    loads[1].wait()
    sign(0, BX - 1, 0, BY)
    loads[2].wait()
    for x in range(BX):
        sign(1, x, BY - 8, 8)
    for k in (0, 4, 5, 6):
        loads[k].wait()

    count = [0]
    edges = {-1: (gx > 0, gy > 0), 1: (gx < 7, gy < 15)}

    def transfer(ref, lead, source, target, sx, sy):
        k = count[0]
        count[0] += 1
        copy = pltpu.make_async_remote_copy(
            src_ref=ref.at[(*lead, *source)], dst_ref=ref.at[(*lead, *target)],
            send_sem=send.at[k], recv_sem=recv.at[k], device_id=neighbour(sx, sy), device_id_type=MESH)
        sends, receives = None, None
        if sx:
            sends, receives = edges[sx][0], edges[-sx][0]
        if sy:
            ys, yr = edges[sy][1], edges[-sy][1]
            sends = ys if sends is None else jnp.logical_and(sends, ys)
            receives = yr if receives is None else jnp.logical_and(receives, yr)
        pl.when(sends)(copy.start)
        return copy, sends, receives

    def finish(copies):
        for copy, sends, receives in copies:
            pl.when(receives)(copy.wait_recv)
            pl.when(sends)(copy.wait_send)

    XS, YS = pl.ds(OX, BX), pl.ds(OY, BY)

    def to_above(ref, lead, axis, width):
        if axis == 0:
            return transfer(ref, lead, (pl.ds(OX + BX - width, width), YS), (pl.ds(OX - width, width), YS), 1, 0)
        return transfer(ref, lead, (XS, pl.ds(BOT - width, width)), (XS, pl.ds(TOP - width, width)), 0, 1)

    def to_below(ref, lead, axis, width):
        if axis == 0:
            return transfer(ref, lead, (pl.ds(OX, width), YS), (pl.ds(OX + BX, width), YS), -1, 0)
        return transfer(ref, lead, (XS, pl.ds(TOP, width)), (XS, pl.ds(BOT, width)), 0, -1)

    def corner(ref, lead, sx, sy):
        xs, xt = (OX + BX - 1, OX - 1) if sx > 0 else (OX, OX + BX)
        ys, yt = (BOT - 1, TOP - 1) if sy > 0 else (TOP, BOT)
        return transfer(ref, lead, (pl.ds(xs, 1), pl.ds(ys, 1)), (pl.ds(xt, 1), pl.ds(yt, 1)), sx, sy)

    def swap(ref, lead):
        return [to_above(ref, lead, 0, 2), to_below(ref, lead, 0, 2), to_above(ref, lead, 1, 2),
                to_below(ref, lead, 1, 2)] + [corner(ref, lead, sx, sy) for sx in (1, -1) for sy in (1, -1)]

    def ahead_z(v):
        rows = v.shape[0]
        at = lax.broadcasted_iota(jnp.int32, (rows, BZ), 1)
        return jnp.where(at == BZ - 1, 0.0, pltpu.roll(v, BZ - 1, 1))

    def behind_z(v):
        rows = v.shape[0]
        at = lax.broadcasted_iota(jnp.int32, (rows, BZ), 1)
        return jnp.where(at == 0, 0.0, pltpu.roll(v, 1, 1))

    def stencil(src, x0, n, segments, emit, advect=True, diffuse=True, unroll=1):
        def start(r, size):
            rows = pl.ds(r, size)
            v = src[x0, rows]
            dx = v - src[x0 - 1, rows]
            parts = [v]
            if diffuse:
                parts.append(cf[0, x0 - 1, rows] * dx)
            if advect:
                parts.append(jnp.minimum(vel[0, x0 - 1, rows], 0.0) * dx)
            return tuple(parts)

        def plane(x, carry):
            done = []
            for (r, size), held in zip(segments, carry):
                rows, up, down = pl.ds(r, size), pl.ds(r + 1, size), pl.ds(r - 1, size)
                v = held[0]
                ahead = src[x + 1, rows]
                dx = ahead - v
                dyu = src[x, up] - v
                dyd = v - src[x, down]
                dz = ahead_z(v) - v
                parts = [ahead]
                dv = fv = None
                if diffuse:
                    fx = cf[0, x, rows] * dx
                    fz = cf[2, x, rows] * dz
                    dv = (fx - held[1]) + (cf[1, x, rows] * dyu - cf[1, x, down] * dyd) + (fz - behind_z(fz))
                    parts.append(fx)
                if advect:
                    u0, u1, u2 = vel[0, x, rows], vel[1, x, rows], vel[2, x, rows]
                    fv = (jnp.maximum(u0, 0.0) * dx + held[-1])
                    fv = fv + (jnp.maximum(u1, 0.0) * dyu + jnp.minimum(vel[1, x, down], 0.0) * dyd)
                    fv = fv + (jnp.maximum(u2, 0.0) * dz + behind_z(jnp.minimum(u2, 0.0) * dz))
                    parts.append(jnp.minimum(u0, 0.0) * dx)
                emit(x, rows, v, fv, dv)
                done.append(tuple(parts))
            return tuple(done)

        carry = tuple(start(r, size) for r, size in segments)
        if unroll >= n:
            for i in range(n):
                carry = plane(x0 + i, carry)
        else:
            lax.fori_loop(x0, x0 + n, plane, carry, unroll=unroll)

    def blocks(src, x0, n, px, segments, emit, advect=True, diffuse=True):
        def at(ref, lead, x, count, r, size):
            return ref[(*lead, pl.ds(x, count), pl.ds(r, size))].reshape(count * size, BZ)

        def one(x):
            for r, size in segments:
                wide = at(src, (), x - 1, px + 2, r, size)
                v = wide[size:-size]
                dx = wide[size:] - wide[:-size]
                dyu = at(src, (), x, px, r + 1, size) - v
                dyd = v - at(src, (), x, px, r - 1, size)
                dz = ahead_z(v) - v
                dv = fv = None
                if diffuse:
                    fx = at(cf, (0,), x - 1, px + 1, r, size) * dx
                    fz = at(cf, (2,), x, px, r, size) * dz
                    fy = at(cf, (1,), x, px, r, size) * dyu - at(cf, (1,), x, px, r - 1, size) * dyd
                    dv = (fx[size:] - fx[:-size]) + fy + (fz - behind_z(fz))
                if advect:
                    u0 = at(vel, (0,), x - 1, px + 1, r, size)
                    u1, u2 = at(vel, (1,), x, px, r, size), at(vel, (2,), x, px, r, size)
                    u1d = at(vel, (1,), x, px, r - 1, size)
                    fv = jnp.maximum(u0[size:], 0.0) * dx[size:] + jnp.minimum(u0[:-size], 0.0) * dx[:-size]
                    fv = fv + (jnp.maximum(u1, 0.0) * dyu + jnp.minimum(u1d, 0.0) * dyd)
                    fv = fv + (jnp.maximum(u2, 0.0) * dz + behind_z(jnp.minimum(u2, 0.0) * dz))
                emit(pl.ds(x, px), pl.ds(r, size), v, fv, dv)

        if n == px:
            one(x0)
        else:
            lax.fori_loop(0, n // px, lambda i, _: (one(x0 + i * px), 0)[1], 0)

    def shaped(x, rows, value):
        return value.reshape(x.size, rows.size, BZ) if isinstance(x, pl.Slice) else value

    def flat(value):
        return value.reshape(-1, BZ)

    WHOLE = ((OY, BY),)
    INNER = ((OY + 8, BY - 16),)
    STRIPS = ((OY, 8), (BOT - 8, 8))
    CORE = tuple((OY + 8 + 24 * i, 24) for i in range(2))
    WIDE7 = tuple((OY - 8 + 40 * i, 40) for i in range(2))
    HALVES = ((OY, BY // 2), (OY + BY // 2, BY // 2))

    def rim(src, emit, width, **kinds):
        ends = HALVES if width == 2 else WHOLE
        blocks(src, OX, width, width, ends, emit, **kinds)
        blocks(src, OX + BX - width, width, width, ends, emit, **kinds)
        blocks(src, OX + width, BX - 2 * width, 10 if width == 1 else 7, STRIPS, emit, **kinds)

    def inner_part(src, emit, width, **kinds):
        n = BX - 2 * width
        stencil(src, OX + width, n, INNER, emit, unroll=UI[width - 1], **kinds)

    def emit_y4(x, rows, v, fv, dv):
        y4[x, rows] = shaped(x, rows, 0.25 * (fv + dv))

    pl.semaphore_wait(barrier, len(friends))
    first = [to_above(cfield, (), 0, 1), to_below(cfield, (), 0, 1), to_above(cfield, (), 1, 1),
             to_below(cfield, (), 1, 1), to_above(cf, (0,), 0, 2), to_above(cf, (1,), 1, 2),
             to_above(vel, (0,), 0, 1), to_above(vel, (1,), 1, 1)]
    later = [to_above(cf, (pl.ds(1, 2),), 0, 1), to_below(cf, (pl.ds(0, 3),), 0, 1),
             to_above(cf, (0,), 1, 1), to_above(cf, (2,), 1, 1), to_below(cf, (pl.ds(0, 3),), 1, 1),
             corner(cf, (pl.ds(0, 2),), 1, 1), corner(cf, (1,), -1, 1), corner(cf, (0,), 1, -1)]
    for o in GROUP_B:
        pl.semaphore_signal(in_sem, inc=1, device_id=device(o), device_id_type=MESH)
    loads[3].wait()
    for x in range(BX):
        if x < BX - 1:
            sign(0, x, 0, BY)
        sign(1, x, 0, BY - 8)
        sign(2, x, 0, BY)
    inner_part(cfield, emit_y4, 1)
    finish(first)
    rim(cfield, emit_y4, 1)
    moved = swap(y4, ())

    def to_w(dst):
        def emit(x, rows, v, fv, dv):
            dst[x, rows] = shaped(x, rows, -dv)
        return emit

    WIDE = ((OY - 8, BY + 16),)

    def clear_outside(ref):
        @pl.when(gx == 0)
        def _():
            ref[OX - 1] = jnp.zeros((EY, BZ), F32)

        @pl.when(gx == 7)
        def _():
            ref[OX + BX] = jnp.zeros((EY, BZ), F32)

        def rows_at(r):
            def body(x, _):
                ref[x, pl.ds(r, 8)] = jnp.zeros((8, BZ), F32)
                return 0
            lax.fori_loop(OX, OX + BX, body, 0, unroll=8)

        pl.when(gy == 0)(lambda: rows_at(TOP - 8))
        pl.when(gy == 15)(lambda: rows_at(BOT))

    def fold(values):
        return jnp.sum(values.reshape(values.shape[0] // 8, 8, BZ), axis=0)

    def moments(y, w):
        zero = jnp.zeros((8, BZ), F32)
        got = (zero,) * 4
        for r, size in HALVES:
            def plane(x, carry, r=r, size=size):
                a0, a1, a2, a3, here = carry
                rows = pl.ds(r, size)
                v = y[x, rows]
                ahead = w[x + 1, rows]
                dx = ahead - here
                dy = w[x, pl.ds(r + 1, size)] - here
                dz = ahead_z(here) - here
                energy = (cf[0, x, rows] * dx) * dx + (cf[1, x, rows] * dy) * dy + (cf[2, x, rows] * dz) * dz
                return (a0 + fold(v * v), a1 + fold(v * here), a2 + fold(here * here), a3 + fold(energy), ahead)

            got = lax.fori_loop(OX, OX + BX, plane, (*got[:4], w[OX, pl.ds(r, size)]), unroll=16)
        return got[:4]

    def send_sums(r, parts):
        row = jnp.zeros((1, BZ), F32)
        for k, part in enumerate(parts):
            total = jnp.sum(jnp.sum(part, axis=0, keepdims=True), axis=1, keepdims=True)
            row = jnp.where(lane[0:1] == k, total, row)
        sums[r, pl.ds(127, 1)] = row
        for k, o in enumerate(EVERYONE):
            pltpu.make_async_remote_copy(
                src_ref=sums.at[r, pl.ds(127, 1)], dst_ref=sums.at[r, pl.ds(k, 1)],
                send_sem=ar_send.at[r], recv_sem=ar_recv.at[r], device_id=device(o), device_id_type=MESH).start()

    def solve(r):
        pltpu.make_async_remote_copy(
            src_ref=sums.at[r, pl.ds(0, 127)], dst_ref=sums.at[r, pl.ds(0, 127)],
            send_sem=ar_send.at[r], recv_sem=ar_recv.at[r], device_id=device(EVERYONE[0]), device_id_type=MESH).wait()
        row = jnp.sum(sums[r], axis=0, keepdims=True)
        m0, k1, k2, k3 = (
            jnp.broadcast_to(jnp.sum(jnp.where(lane[0:1] == k, row, 0.0), axis=1, keepdims=True), (8, BZ))
            for k in range(4))
        h = 0.25
        alpha = m0 / (m0 + h * k1)
        rho = k1 / m0
        ss = k2 - rho * k1
        sls = k3 - 2.0 * rho * k2 + rho * (rho * k1)
        beta = (alpha * h) * (alpha * h) * (ss / m0)
        under = ss * (1.0 - beta / alpha) + h * sls
        second = jnp.where(under > 0.0, jnp.clip(ss / under, 0.0, 1.0), 0.0)
        return alpha + second * (alpha * h * rho + beta), -second * alpha * h

    def full(scalar, size):
        return jnp.concatenate([scalar] * (size // 8), axis=0)

    def held(ref, x, px, r, size, dx=0, dr=0):
        return ref[pl.ds(x + dx, px), pl.ds(r + dr, size)].reshape(px * size, BZ)

    def d_weights(x, px, r, size):
        return (held(cf.at[0], x, px, r, size), held(cf.at[0], x, px, r, size, -1),
                held(cf.at[1], x, px, r, size), held(cf.at[1], x, px, r, size, 0, -1),
                held(up_z, x, px, r, size), held(down_z, x, px, r, size), held(centre, x, px, r, size))

    def s_weights(x, px, r, size):
        return tuple(held(sc.at[k], x, px, r, size, -OX, -OY) for k in range(7))

    def seven(src, weights, emit, x, px, r, size, before, here, after):
        north, south = held(src, x, px, r, size, 0, 1), held(src, x, px, r, size, 0, -1)
        up, down = pltpu.roll(here, BZ - 1, 1), pltpu.roll(here, 1, 1)
        results = []
        for weight in weights:
            e, w, n, s, u, d, c = weight(x, px, r, size)
            results.append((e * after + w * before) + (n * north + s * south) + (u * up + d * down) - c * here)
        emit(x, px, r, size, here, *results)

    def sweep7(src, x0, n, segments, weights, emit, unroll):
        for r, size in segments:
            def plane(x, carry, r=r, size=size):
                before, here = carry
                after = held(src, x, 1, r, size, 1)
                seven(src, weights, emit, x, 1, r, size, before, here, after)
                return here, after

            lax.fori_loop(x0, x0 + n, plane, (held(src, x0, 1, r, size, -1), held(src, x0, 1, r, size)), unroll=unroll)

    def blocks7(src, x0, n, px, segments, weights, emit):
        def one(x):
            for r, size in segments:
                wide = held(src, x - 1, px + 2, r, size)
                seven(src, weights, emit, x, px, r, size, wide[:-2 * size], wide[size:-size], wide[2 * size:])

        if n == px:
            one(x0)
        else:
            lax.fori_loop(0, n // px, lambda i, _: (one(x0 + i * px), 0)[1], 0)

    def put(ref, x, px, r, size, value, dx=0, dr=0):
        ref[pl.ds(x + dx, px), pl.ds(r + dr, size)] = value.reshape(px, size, BZ)

    def advance(y, w, qr, g, r):
        def emit_q(x, px, r, size, v, sv):
            put(qr.at[0], x, px, r, size, sv)

        def emit_r(x, px, r, size, v, sv, dv):
            put(qr.at[1], x, px, r, size, sv)
            put(g, x, px, r, size, dv)

        def emit_s(x, px, r, size, v, sv):
            put(qr.at[1], x, px, r, size, sv)

        def emit_g(x, px, r, size, v, dv):
            put(g, x, px, r, size, dv)

        def rim7(src, weights, emit):
            blocks7(src, OX, 2, 2, HALVES, weights, emit)
            blocks7(src, OX + BX - 2, 2, 2, HALVES, weights, emit)
            blocks7(src, OX + 2, BX - 4, 7, STRIPS, weights, emit)

        both = (s_weights, d_weights)
        rim7(y, (s_weights,), emit_q)
        copies = swap(qr, (0,))
        send_sums(r, moments(y, w))
        rim7(w, (s_weights,), emit_s)
        copies += swap(qr, (1,))
        if r == 0:
            prepare_d(OX, BX, OY, BY)
        rim7(w, (d_weights,), emit_g)
        sweep7(y, OX + 2, BX - 4, CORE, (s_weights,), emit_q, UNROLL[0])
        sweep7(w, OX + 2, BX - 4, CORE, both, emit_r, UNROLL[0])
        return copies

    def laplacian7(src, dst):
        def emit(x, px, r, size, v, dv):
            put(dst, x, px, r, size, -dv)

        sweep7(src, OX - 1, BX + 2, WIDE7, (d_weights,), emit, UNROLL[1])

    def prepare_s():
        def body(x, _):
            for r, size in HALVES:
                a = [vel[d, x, pl.ds(r, size)] for d in range(3)]
                k = [0.25 * cf[d, x, pl.ds(r, size)] for d in range(3)]
                e, n, u = (0.5 * jnp.maximum(a[d], 0.0) + k[d] for d in range(3))
                w = 0.25 * cf[0, x - 1, pl.ds(r, size)] - 0.5 * jnp.minimum(vel[0, x - 1, pl.ds(r, size)], 0.0)
                s = 0.25 * cf[1, x, pl.ds(r - 1, size)] - 0.5 * jnp.minimum(vel[1, x, pl.ds(r - 1, size)], 0.0)
                d = behind_z(k[2] - 0.5 * jnp.minimum(a[2], 0.0))
                at = lax.broadcasted_iota(jnp.int32, (size, BZ), 1)
                values = (e, w, n, s, jnp.where(at == BZ - 1, 0.0, u), d, (e + w) + (n + s) + (u + d))
                for i, value in enumerate(values):
                    sc[i, x - OX, pl.ds(r - OY, size)] = value
            return 0

        lax.fori_loop(OX, OX + BX, body, 0, unroll=2)

    def prepare_d(x0, n, r, size):
        def body(x, _):
            rows = pl.ds(r, size)
            k = cf[2, x, rows]
            d = behind_z(k)
            at = lax.broadcasted_iota(jnp.int32, (size, BZ), 1)
            up_z[x, rows] = jnp.where(at == BZ - 1, 0.0, k)
            down_z[x, rows] = d
            centre[x, rows] = ((cf[0, x, rows] + cf[0, x - 1, rows]) + (cf[1, x, rows] + cf[1, x, pl.ds(r - 1, size)])
                               + (k + d))
            return 0

        lax.fori_loop(x0, x0 + n, body, 0, unroll=8 if n > 1 else 1)

    def everywhere(fn):
        def body(x, _):
            fn(x, pl.ds(OY - 8, BY + 16))
            return 0
        lax.fori_loop(0, NX, body, 0, unroll=4)

    def block(fn, unroll=4):
        def body(x, _):
            fn(x, pl.ds(OY, BY))
            return 0
        lax.fori_loop(OX, OX + BX, body, 0, unroll=unroll)

    inner_part(y4, to_w(w4), 1, advect=False)
    prepare_s()
    finish(moved)
    finish(later)
    blocks(y4, OX - 1, 2, 2, WIDE, to_w(w4), advect=False)
    blocks(y4, OX + BX - 1, 2, 2, WIDE, to_w(w4), advect=False)
    blocks(y4, OX + 1, BX - 2, 5, ((OY - 8, 16), (BOT - 8, 16)), to_w(w4), advect=False)
    clear_outside(w4)
    pl.semaphore_wait(in_sem, len(GROUP_B))
    moved = advance(y4, w4, qr4, g4, 0)
    prepare_d(OX - 1, 1, OY, BY)
    prepare_d(OX + BX, 1, OY, BY)
    prepare_d(OX, BX, OY - 8, 8)
    prepare_d(OX, BX, BOT, 8)
    finish(moved)
    a4, c4 = solve(0)

    def base2(x, rows):
        size = rows.size
        a, c = full(a4, size), full(c4, size)
        qr3[2, x, rows] = (1.4 * y4[x, rows] + a * (0.6 * qr4[0, x, rows] - 0.2 * w4[x, rows])
                           + c * (0.6 * qr4[1, x, rows] + 0.2 * g4[x, rows]))

    def few(x0, n):
        for i in range(n):
            base2(x0 + i, pl.ds(OY, BY))

    def strips(i, _):
        for k in range(7):
            base2(OX + 2 + 7 * i + k, pl.ds(OY, 8))
            base2(OX + 2 + 7 * i + k, pl.ds(BOT - 8, 8))
        return 0

    few(OX, 2)
    few(OX + BX - 2, 2)
    lax.fori_loop(0, 4, strips, 0)
    moved2 = swap(qr3, (2,))

    def make_y3(x, rows):
        a, c = full(a4, rows.size), full(c4, rows.size)
        y3[x, rows] = y4[x, rows] + a * qr4[0, x, rows] + c * qr4[1, x, rows]

    everywhere(make_y3)
    laplacian7(y3, w3)
    clear_outside(w3)
    moved = advance(y3, w3, qr3, g3, 1)
    lax.fori_loop(OX + 2, OX + BX - 2, lambda x, _: (base2(x, pl.ds(OY + 8, BY - 16)), 0)[1], 0, unroll=4)
    finish(moved2)
    finish(moved)
    a3, c3 = solve(1)

    def make_y2(x, rows):
        a, c = full(a3, rows.size), full(c3, rows.size)
        y2[x, rows] = qr3[2, x, rows] + a * qr3[0, x, rows] + c * qr3[1, x, rows]

    everywhere(make_y2)
    laplacian7(y2, w2)
    clear_outside(w2)
    send_sums(2, moments(y2, w2))

    def emit_t1(x, px, r, size, v, sv):
        put(t1, x, px, r, size, v + sv, -OX, -OY)

    def emit_t2(x, px, r, size, v, sv):
        put(t2, x, px, r, size, v + sv, -OX, -OY)

    sweep7(y2, OX, BX, HALVES, (s_weights,), emit_t1, UNROLL[2])
    sweep7(w2, OX, BX, HALVES, (s_weights,), emit_t2, UNROLL[2])

    def base1(x, rows):
        size = rows.size
        a, c, a_, c_ = full(a4, size), full(c4, size), full(a3, size), full(c3, size)
        total = cfield[x, rows] + 0.6 * y4[x, rows]
        total = total + a * (y4[x, rows] + 0.4 * qr4[0, x, rows] - 0.05 * w4[x, rows])
        total = total + c * (w4[x, rows] + 0.4 * qr4[1, x, rows] + 0.05 * g4[x, rows])
        total = total + a_ * (y3[x, rows] + 0.5 * qr3[0, x, rows] - 0.125 * w3[x, rows])
        total = total + c_ * (w3[x, rows] + 0.5 * qr3[1, x, rows] + 0.125 * g3[x, rows])
        b1[x - OX] = total

    block(base1)
    a2, c2 = solve(2)
    def body(x, _):
        out[x] = b1[x] + full(a2, BY) * t1[x] + full(c2, BY) * t2[x]
        return 0

    lax.fori_loop(0, BX, body, 0, unroll=8)


COPIES = 80


def local(cotangent, speed, coeff, dirs):
    ext = pltpu.VMEM(EXT, F32)
    plain = pltpu.VMEM((BX, BY, BZ), F32)

    def stack(n):
        return pltpu.VMEM((n, *EXT), F32)

    anywhere = pl.BlockSpec(memory_space=pl.ANY)
    return pl.pallas_call(
        kernel,
        name="adjoint_step",
        out_shape=jax.ShapeDtypeStruct((BX, BY, BZ), F32),
        in_specs=[anywhere] * 4,
        out_specs=pl.BlockSpec(memory_space=pltpu.VMEM),
        scratch_shapes=[
            ext, stack(3), stack(3), ext, ext, ext, stack(2), ext, ext, ext, stack(3), ext, ext,
            plain, plain, plain, pltpu.VMEM((7, BX, BY, BZ), F32), ext, ext, ext, pltpu.VMEM((3, BX, BY), jnp.int32), pltpu.VMEM((128, 128), F32), pltpu.VMEM((3, 128, BZ), F32),
            pltpu.SemaphoreType.DMA((8,)), pltpu.SemaphoreType.DMA((COPIES,)), pltpu.SemaphoreType.DMA((COPIES,)),
            pltpu.SemaphoreType.DMA((3,)), pltpu.SemaphoreType.DMA((3,)), pltpu.SemaphoreType.REGULAR,
        ],
        compiler_params=pltpu.CompilerParams(
            collective_id=0, has_side_effects=True, vmem_limit_bytes=57 * 1024 * 1024),
    )(cotangent, speed, coeff, dirs)


def solution(mesh):
    placed = (P("gx", "gy", None), P(None, "gx", "gy", None), P(None, "gx", "gy", None), P(None, "gx", "gy"))
    return jax.shard_map(local, mesh=mesh, in_specs=placed, out_specs=P("gx", "gy", None), check_vma=False)
```
